32 devices in a mesh: dp: 8 (over z, x), tensor: 4 (over y, core).
Axes of the slice: x: 2, y: 2, z: 4, core: 2. Of those that a mesh axis runs over, the one named last changes fastest.
Arguments:
- logits: bfloat16 [16, 128, 19456], P('dp', None, 'tensor'), may hold values from -110 to 290
- token_ids: int32 [16, 128], P('dp'), may hold values from 0 to 19455
- response_mask: int32 [16, 128], P('dp'), may hold values 0 or 1
- lengths: int32 [16], P('dp'), may hold values from 16 to 128
- prompt_of: int32 [16], P('dp'), may hold values from 0 to 1, as said below
- old_logprob: float32 [16, 128], P('dp'), may hold values from -14 to -10
- ref_logprob: bfloat16 [16, 128], P(None, 'dp'), may hold values from -14 to -10
- advantages: float32 [16, 128], P('dp'), may hold values from -8 to 8
- returns: float32 [16, 128], P('dp'), may hold values from -6 to 6
- critic_hidden: bfloat16 [16, 128, 5120], P(None, 'dp', 'tensor'), may hold values from -6 to 6
- value_weight: bfloat16 [5120], P('tensor'), may hold values from -0.078125 to 0.078125
Outputs:
- token_loss: float32 [16, 128], P('dp')
- critic_grad: bfloat16 [16, 128, 5120], P(None, 'dp', 'tensor')
The draws below stay inside these ranges and needn't reach their ends.
Inputs may be any that keep to these rules, and one draw needn't show every extreme that they name: `prompt_of`: each of the 2 prompts is named by exactly 8 sequences.
All inputs are finite; a program needn't handle non-finite values. No bound on the sum of `response_mask` on one device may be relied on, other than what follows from the above.
Results may differ from the reference program's by a relative error of at most 0.001.
Values may be sent and summed in bfloat16 or wider, within the bound.
No kernel may reach another device: no remote copies, remote signals or barrier semaphores. Data moves between devices by JAX's collectives and lax.ppermute only.
A program may use at most 64 MiB of HBM per device.

```python
import math
import jax
import jax.numpy as jnp
import numpy as np
from jax import lax

D = 5120
LEN = 128
RESPONSES = 8
BATCH = 16
VOCAB = 19456
PROMPTS = 2


def draw_logits(key, part):
    first_key = jax.random.fold_in(key, 0)
    full_shape = (BATCH, LEN, VOCAB)
    values = 1.5 * jax.random.truncated_normal(first_key, -6.0, 6.0, full_shape, jnp.float32)
    return values.astype(jnp.bfloat16)


def draw_prompt_of(key, part):
    order = jax.random.permutation(jax.random.fold_in(key, 7), BATCH)
    return (order // RESPONSES).astype(jnp.int32)


def plant(result, rng, least, high):
    longest = result.shape.index(max(result.shape))
    spots = []
    for shift in (0, 1):
        where = [jax.random.randint(jax.random.fold_in(rng, axis), (), 0, length) for axis, length in enumerate(result.shape)]
        where[longest] = (where[longest] + shift) % result.shape[longest]
        spots.append(tuple(where))
    return result.at[spots[0]].set(least).at[spots[1]].set(high)


def level_of(stream_key, shape, cuts, low, top_value):
    factor_of, own = 1.0, jax.random.fold_in(stream_key, 6)
    for dim, parts in cuts:
        steps = jnp.exp(jax.random.uniform(jax.random.fold_in(own, dim), (parts,), jnp.float32, low / len(cuts), top_value / len(cuts)))
        factor_of = factor_of * jnp.repeat(steps, shape[dim] // parts).reshape([-1 if axis == dim else 1 for axis in range(len(shape))])
    return factor_of


def rank_bounds(number_of, slope):
    weights = [(1 << 20) // math.isqrt(grade ** slope) + 1 for grade in range(1, number_of + 1)]
    spread = 1 + sum(weights) // (1 << 30)
    return np.cumsum(np.array([max(1, weight // spread) for weight in weights]))


def ranked(own_key, extent, count, slope):
    grid = rank_bounds(count, slope)
    lot = jax.random.randint(jax.random.fold_in(own_key, 1), extent, 0, int(grid[count - 1]))
    rank = jnp.searchsorted(jnp.asarray(grid, jnp.int32), lot, side="right")
    return jax.random.permutation(jax.random.fold_in(own_key, 2), count)[rank].astype(jnp.int32)


def gaussian(stream_key, shape, scale, most, pieces=(), kind=jnp.bfloat16):
    result = scale * jax.random.normal(stream_key, shape, jnp.float32)
    if pieces:
        result = result * level_of(stream_key, shape, pieces, -0.22, 0.18)
    return jnp.clip(result, -most, most).astype(kind)


def setup_inputs(seed: int = 0) -> dict:
    keys = jax.random.split(jax.random.key(seed), 12)
    return {
        "logits": draw_logits(jax.random.fold_in(keys[11], 71), 0),
        "token_ids": plant(ranked(keys[1], (BATCH, LEN), VOCAB, 2), jax.random.fold_in(keys[1], 3), 0, VOCAB - 1).astype(jnp.int32),
        "response_mask": plant((jax.random.randint(keys[2], (BATCH, LEN), 0, 8) < 7).astype(jnp.int32), jax.random.fold_in(keys[2], 1), 0, 1),
        "lengths": plant(jax.random.randint(keys[3], (BATCH,), LEN // 8, LEN + 1), jax.random.fold_in(keys[3], 1), LEN // 8, LEN).astype(jnp.int32),
        "prompt_of": draw_prompt_of(jax.random.fold_in(keys[11], 71), 0),
        "old_logprob": jnp.clip(-14.0 + 4.0 * jax.random.uniform(keys[5], (BATCH, LEN), jnp.float32) ** level_of(keys[5], (BATCH, LEN), ((0, 8),), -0.2, 0.2), -14.0, -10.0),
        "ref_logprob": jnp.clip(-14.0 + 4.0 * jax.random.uniform(keys[6], (BATCH, LEN), jnp.float32) ** level_of(keys[6], (BATCH, LEN), ((1, 8),), -0.2, 0.2), -14.0, -10.0).astype(jnp.bfloat16),
        "advantages": gaussian(keys[7], (BATCH, LEN), 2.0, 8.0, ((0, 8),), jnp.float32),
        "returns": gaussian(keys[8], (BATCH, LEN), 1.0, 6.0, ((0, 8),), jnp.float32),
        "critic_hidden": gaussian(keys[9], (BATCH, LEN, D), 1.0, 6.0, ((1, 8), (2, 4))),
        "value_weight": gaussian(keys[10], (D,), D ** -0.5, 0.078125, ((0, 4),)),
    }


def token_logprob(inputs):
    row_block, row_ids = inputs
    row_max = lax.optimization_barrier(jnp.max(row_block, axis=1)).astype(jnp.float32)
    exp_total = lax.optimization_barrier(jnp.sum(jnp.exp(row_block.astype(jnp.float32) - row_max[:, None]), axis=1))
    picked = jnp.take_along_axis(row_block, row_ids[:, None].astype(jnp.int32), axis=1)[:, 0].astype(jnp.float32)
    return picked - (row_max + jnp.log(exp_total))

def reference(logits, token_ids, response_mask, lengths, prompt_of, old_logprob, ref_logprob, advantages, returns, critic_hidden, value_weight):
    highest = lax.Precision.HIGHEST
    logprob = lax.map(token_logprob, (logits, token_ids))
    head_weight = value_weight.astype(jnp.float32)
    value_pred = jnp.einsum('bld,d->bl', critic_hidden.astype(jnp.float32), head_weight)
    position = jnp.arange(LEN, dtype=jnp.int32)
    live_mask = (response_mask * (position[None, :] < lengths[:, None]).astype(jnp.int32)).astype(jnp.float32)
    prompt_hot = (prompt_of[:, None] == jnp.arange(PROMPTS, dtype=jnp.int32)[None, :]).astype(jnp.float32)
    seq_tokens = lax.optimization_barrier(jnp.sum(live_mask, axis=1))
    seq_total = lax.optimization_barrier(jnp.sum(live_mask * advantages, axis=1))
    count_floor = jnp.maximum(jnp.dot(seq_tokens, prompt_hot, precision=highest), 1.0)
    prompt_mean = jnp.dot(seq_total, prompt_hot, precision=highest) / count_floor
    row_mean = jnp.dot(prompt_hot, prompt_mean, precision=highest)
    centered = advantages - row_mean[:, None]
    seq_square = lax.optimization_barrier(jnp.sum(live_mask * centered * centered, axis=1))
    prompt_var = jnp.dot(seq_square, prompt_hot, precision=highest) / count_floor
    row_scale = 1.0 / jnp.sqrt(jnp.dot(prompt_hot, prompt_var, precision=highest) + 1.0)
    whitened = centered * row_scale[:, None]
    prob_ratio = jnp.exp(jnp.clip(logprob - old_logprob, -20.0, 20.0))
    surrogate = jnp.maximum(-whitened * prob_ratio, -whitened * jnp.clip(prob_ratio, 0.8, 1.2))
    surrogate = jnp.where(whitened < 0.0, jnp.minimum(surrogate, -3.0 * whitened), surrogate)
    ref_drift = jnp.clip(ref_logprob.astype(jnp.float32) - logprob, -20.0, 20.0)
    penalty = jnp.clip(jnp.exp(ref_drift) - ref_drift - 1.0, -10.0, 10.0)
    value_error = value_pred - returns
    token_loss = live_mask * (surrogate + 0.1 * penalty + 0.25 * value_error * value_error)
    grad_coeff = 32.0 * live_mask * value_error
    critic_grad = (grad_coeff[:, :, None] * head_weight[None, None, :]).astype(jnp.bfloat16)
    return (token_loss, critic_grad)
```

```python
import jax
import jax.numpy as jnp
from jax import lax
from jax.sharding import PartitionSpec as P


def per_device(
    logits,
    token_ids,
    response_mask,
    lengths,
    prompt_of,
    old_logprob,
    ref_logprob,
    advantages,
    returns,
    critic_hidden,
    value_weight,
):
    seq_rows, seq_len, vocab_width = logits.shape
    all_seqs, tile_len, feat_count = critic_hidden.shape
    dp_size = lax.axis_size("dp")
    tensor_size = lax.axis_size("tensor")

    tile_rows = critic_hidden.reshape(all_seqs * tile_len, feat_count)
    tile_part = jnp.dot(tile_rows, value_weight, preferred_element_type=jnp.float32).reshape(
        all_seqs, tile_len
    )

    position = lax.broadcasted_iota(jnp.int32, (seq_rows, seq_len), 1)
    live_mask = (response_mask * (position < lengths[:, None]).astype(jnp.int32)).astype(
        jnp.float32
    )
    moments = jnp.stack(
        [
            jnp.sum(live_mask, axis=1),
            jnp.sum(live_mask * advantages, axis=1),
            jnp.sum(live_mask * advantages * advantages, axis=1),
            prompt_of.astype(jnp.float32),
        ],
        axis=1,
    )

    def by_tile(rows):
        return rows.reshape(seq_rows, dp_size, tile_len).transpose(1, 0, 2)

    def by_group(tile):
        return tile.reshape(dp_size, seq_rows, tile_len)

    block = jnp.concatenate(
        [
            by_group(tile_part),
            by_group(ref_logprob.astype(jnp.float32)),
            by_tile(returns),
            by_tile(live_mask),
            jnp.broadcast_to(moments[None], (dp_size, seq_rows, 4)),
        ],
        axis=2,
    )
    width = block.shape[2]
    send = jnp.broadcast_to(block[:, None], (dp_size, tensor_size, seq_rows, width)).reshape(
        dp_size * tensor_size, seq_rows, width
    )
    received = lax.all_to_all(send, ("dp", "tensor"), 0, 0, tiled=True).reshape(
        dp_size, tensor_size, seq_rows, width
    )

    local_top = jnp.max(logits, axis=2).astype(jnp.float32)
    vocab_start = lax.axis_index("tensor") * vocab_width
    shifted = token_ids - vocab_start
    column = lax.broadcasted_iota(jnp.int32, logits.shape, 2)
    wide = logits.astype(jnp.float32)
    local_sum = jnp.sum(jnp.exp(wide - local_top[:, :, None]), axis=2)
    local_target = jnp.sum(jnp.where(column == shifted[:, :, None], wide, 0.0), axis=2)

    shard_stats = lax.all_gather(
        jnp.stack(
            [local_top, local_sum, local_target, tile_part.reshape(seq_rows, seq_len)]
        ),
        "tensor",
    )
    tops = shard_stats[:, 0]
    row_max = jnp.max(tops, axis=0)
    total_sum = jnp.sum(shard_stats[:, 1] * jnp.exp(tops - row_max[None]), axis=0)
    target_logit = jnp.sum(shard_stats[:, 2], axis=0)
    tile_value = jnp.sum(shard_stats[:, 3], axis=0).reshape(all_seqs, tile_len)
    logprob = target_logit - (row_max + jnp.log(total_sum))

    def to_rows(blocks):
        return blocks.transpose(1, 0, 2).reshape(seq_rows, seq_len)

    first = received[:, 0]
    value_pred = to_rows(jnp.sum(received[:, :, :, :tile_len], axis=1))
    ref_rows = to_rows(first[:, :, tile_len : 2 * tile_len])
    tile_returns = first[:, :, 2 * tile_len : 3 * tile_len].reshape(all_seqs, tile_len)
    tile_mask = first[:, :, 3 * tile_len : 4 * tile_len].reshape(all_seqs, tile_len)
    seq_moments = first[:, :, 4 * tile_len :].reshape(all_seqs, 4)

    same = (prompt_of.astype(jnp.float32)[:, None] == seq_moments[None, :, 3]).astype(jnp.float32)
    count = jnp.sum(same * seq_moments[None, :, 0], axis=1)
    total = jnp.sum(same * seq_moments[None, :, 1], axis=1)
    square = jnp.sum(same * seq_moments[None, :, 2], axis=1)
    count_floor = jnp.maximum(count, 1.0)
    prompt_mean = total / count_floor
    prompt_var = (square - prompt_mean * total) / count_floor
    row_scale = lax.rsqrt(prompt_var + 1.0)
    whitened = (advantages - prompt_mean[:, None]) * row_scale[:, None]

    prob_ratio = jnp.exp(jnp.clip(logprob - old_logprob, -20.0, 20.0))
    surrogate = jnp.maximum(-whitened * prob_ratio, -whitened * jnp.clip(prob_ratio, 0.8, 1.2))
    surrogate = jnp.where(whitened < 0.0, jnp.minimum(surrogate, -3.0 * whitened), surrogate)
    ref_drift = jnp.clip(ref_rows - logprob, -20.0, 20.0)
    penalty = jnp.clip(jnp.exp(ref_drift) - ref_drift - 1.0, -10.0, 10.0)
    value_error = value_pred - returns
    token_loss = live_mask * (surrogate + 0.1 * penalty + 0.25 * value_error * value_error)

    head_weight = value_weight.astype(jnp.float32)
    grad_coeff = 32.0 * tile_mask * (tile_value - tile_returns)
    critic_grad = (grad_coeff[:, :, None] * head_weight[None, None, :]).astype(jnp.bfloat16)
    return (token_loss, critic_grad)


def solution(mesh):
    in_specs = (
        P("dp", None, "tensor"),
        P("dp", None),
        P("dp", None),
        P("dp"),
        P("dp"),
        P("dp", None),
        P(None, "dp"),
        P("dp", None),
        P("dp", None),
        P(None, "dp", "tensor"),
        P("tensor"),
    )
    out_specs = (P("dp", None), P(None, "dp", "tensor"))
    return jax.shard_map(
        per_device, mesh=mesh, in_specs=in_specs, out_specs=out_specs, check_vma=False
    )
```

```python
import functools

import jax
import jax.numpy as jnp
from jax import lax
from jax.experimental import pallas as pl
from jax.experimental.pallas import tpu as pltpu
from jax.sharding import PartitionSpec as P

LANES = 128
F32 = jnp.float32


def fold(x, period):
    shift = LANES // 2
    while shift >= period:
        x = x + pltpu.roll(x, shift, 1)
        shift //= 2
    return x


def in_hbm(*arrays):
    return [pltpu.with_memory_space_constraint(x, pltpu.HBM) for x in arrays]


def live_row(rmask_ref, len_ref, s):
    position = lax.broadcasted_iota(jnp.int32, (1, LANES), 1)
    return jnp.where(position < len_ref[s], rmask_ref[s : s + 1, :], 0).astype(F32)


def pre_kernel(
    dims, len_hbm, prompt_hbm, critic_hbm, w_hbm, refl_hbm, ret_hbm, rmask_hbm, adv_hbm,
    send_hbm, part_ref,
    len_ref, prompt_ref, critic_ref, w_ref, reflp_ref, ret_ref, rmask_ref, adv_ref, send_ref,
    wide_ref, sems,
):
    dp, tn, rows, tl = dims
    feat = critic_ref.shape[1]
    pairs = (
        (w_hbm, w_ref), (critic_hbm, critic_ref), (rmask_hbm, rmask_ref), (adv_hbm, adv_ref),
        (ret_hbm, ret_ref), (refl_hbm, reflp_ref), (len_hbm, len_ref), (prompt_hbm, prompt_ref),
    )
    copies = [pltpu.make_async_copy(a, b, sems.at[k]) for k, (a, b) in enumerate(pairs)]
    for copy in copies:
        copy.start()
    for copy in copies[2:]:
        copy.wait()
    wide_ref[:, 0:tl] = reflp_ref[...].astype(F32)
    sub = lax.broadcasted_iota(jnp.int32, (dp, LANES), 0)
    lane = lax.broadcasted_iota(jnp.int32, (dp, LANES), 1)
    slot = lane // tl
    blocks = []
    for s in range(rows):
        live = live_row(rmask_ref, len_ref, s)
        adv = adv_ref[s : s + 1, :]
        gain = live * adv
        refs = jnp.where(slot == 0, wide_ref[pl.ds(s, dp, stride=rows), :], 0.0)
        rets = jnp.where(slot == sub, jnp.broadcast_to(ret_ref[s : s + 1, :], (dp, LANES)), 0.0)
        lives = jnp.where(slot == sub, jnp.broadcast_to(live, (dp, LANES)), 0.0)
        block = jnp.where(slot == 1, fold(refs, tl), 0.0)
        block = jnp.where(slot == 2, fold(rets, tl), block)
        block = jnp.where(slot == 3, fold(lives, tl), block)
        block = jnp.where(lane == 4 * tl, jnp.sum(live, axis=1, keepdims=True), block)
        block = jnp.where(lane == 4 * tl + 1, jnp.sum(gain, axis=1, keepdims=True), block)
        block = jnp.where(lane == 4 * tl + 2, jnp.sum(gain * adv, axis=1, keepdims=True), block)
        block = jnp.where(lane == 4 * tl + 3, prompt_ref[s].astype(F32), block)
        blocks.append(block)
    for copy in copies[:2]:
        copy.wait()
    weights = jnp.broadcast_to(w_ref[...][None, :], (16, feat))
    flat = lax.dot_general(
        weights, critic_ref[...], (((1,), (1,)), ((), ())), preferred_element_type=F32
    )
    for h in range(rows):
        part_ref[h : h + 1, :] = flat[0:1, h * LANES : (h + 1) * LANES]
    for s in range(rows):
        value = jnp.zeros((dp, LANES), F32)
        for h in range(rows):
            line = jnp.broadcast_to(flat[0:1, h * LANES : (h + 1) * LANES], (dp, LANES))
            value = jnp.where((h * LANES + lane) // tl == sub * rows + s, line, value)
        block = jnp.where(slot == 0, fold(value, tl), blocks[s])
        for j in range(tn):
            send_ref[pl.ds(j * rows + s, dp, stride=tn * rows), :] = block
    out = pltpu.make_async_copy(send_ref, send_hbm, sems.at[len(pairs)])
    out.start()
    out.wait()


def stats_kernel(
    ids_hbm, part_ref, logits_hbm, out_ref,
    logits_ref, ids_ref, id_ref, top_ref, sum_ref, hit_ref, sems, ids_sem,
):
    rows, tokens, width = logits_ref.shape
    steps = sems.shape[1]
    step = tokens // steps
    copies = [
        [
            pltpu.make_async_copy(
                logits_hbm.at[s, pl.ds(k * step, step)],
                logits_ref.at[s, pl.ds(k * step, step)],
                sems.at[s, k],
            )
            for k in range(steps)
        ]
        for s in range(rows)
    ]
    ids_copy = pltpu.make_async_copy(ids_hbm, ids_ref, ids_sem)
    ids_copy.start()
    for row in copies:
        for copy in row:
            copy.start()
    start = lax.axis_index("tensor") * width
    lane = lax.broadcasted_iota(jnp.int32, (tokens, LANES), 1)
    ids_copy.wait()
    for s in range(rows):
        ids = jnp.broadcast_to(ids_ref[s : s + 1, :].astype(F32), (LANES, tokens))
        shifted = jnp.transpose(ids).astype(jnp.int32) - start
        id_ref[s] = jnp.where(lane == (shifted & (LANES - 1)), shifted >> 7, -1)
    for s in range(rows):
        for k in range(steps):
            copies[s][k].wait()
            at = slice(k * step, (k + 1) * step)
            top = logits_ref[s, at, 0:LANES]
            for c in range(1, width // LANES):
                top = jnp.maximum(top, logits_ref[s, at, c * LANES : (c + 1) * LANES])
            top = jnp.max(top.astype(F32), axis=1, keepdims=True)
            hot = id_ref[s, at, :]
            total = jnp.zeros((step, LANES), F32)
            hit = jnp.zeros((step, LANES), F32)
            for c in range(width // LANES):
                x = logits_ref[s, at, c * LANES : (c + 1) * LANES].astype(F32)
                total = total + jnp.exp(x - top)
                hit = jnp.where(hot == c, x, hit)
            top_ref[at, :] = jnp.broadcast_to(top, (step, LANES))
            sum_ref[at, :] = total
            hit_ref[at, :] = hit
        out_ref[s : s + 1, :] = jnp.transpose(top_ref[...])[0:1, :]
        out_ref[rows + s : rows + s + 1, :] = jnp.sum(
            jnp.transpose(sum_ref[...]), axis=0, keepdims=True
        )
        out_ref[2 * rows + s : 2 * rows + s + 1, :] = jnp.sum(
            jnp.transpose(hit_ref[...]), axis=0, keepdims=True
        )
    out_ref[3 * rows : 4 * rows, :] = part_ref[...]


def post_kernel(
    dims, len_ref, prompt_ref, recv_ref, stats_ref, w_ref, old_ref, adv_ref, ret_ref, rmask_ref,
    loss_ref, grad_ref,
):
    dp, tn, rows, tl = dims
    seqs = dp * rows
    sub = lax.broadcasted_iota(jnp.int32, (dp, LANES), 0)
    lane = lax.broadcasted_iota(jnp.int32, (dp, LANES), 1)
    slot = lane // tl

    def pick(x, k):
        return fold(jnp.where(slot == k, x, 0.0), tl)

    def down(x):
        return jnp.sum(x, axis=0, keepdims=True)

    firsts, values, refs = [], [], []
    flat_ret = [jnp.zeros((1, LANES), F32) for _ in range(rows)]
    flat_live = [jnp.zeros((1, LANES), F32) for _ in range(rows)]
    for s in range(rows):
        parts = [recv_ref[pl.ds(j * rows + s, dp, stride=tn * rows), :] for j in range(tn)]
        first = parts[0]
        every = sum(parts[1:], first)
        firsts.append(first)
        values.append(down(jnp.where(slot == sub, pick(every, 0), 0.0)))
        refs.append(down(jnp.where(slot == sub, pick(first, 1), 0.0)))
        tile_ret, tile_live = pick(first, 2), pick(first, 3)
        for h in range(rows):
            here = (h * LANES + lane) // tl == sub * rows + s
            flat_ret[h] += down(jnp.where(here, tile_ret, 0.0))
            flat_live[h] += down(jnp.where(here, tile_live, 0.0))

    seq_sub = lax.broadcasted_iota(jnp.int32, (seqs, LANES), 0)
    seq_lane = lax.broadcasted_iota(jnp.int32, (seqs, LANES), 1)
    coeff = jnp.zeros((seqs, LANES), F32)
    for h in range(rows):
        tile_value = stats_ref[0, 3 * rows + h : 3 * rows + h + 1, :]
        for j in range(1, tn):
            tile_value += stats_ref[j, 3 * rows + h : 3 * rows + h + 1, :]
        line = 32.0 * flat_live[h] * (tile_value - flat_ret[h])
        here = (h * LANES + seq_lane) // tl == seq_sub
        coeff = jnp.where(here, jnp.broadcast_to(line, (seqs, LANES)), coeff)
    columns = jnp.transpose(fold(coeff, tl))
    weights = w_ref[...].astype(F32)
    for b in range(seqs):
        grad_ref[b] = (columns[0:tl, b : b + 1] * weights).astype(grad_ref.dtype)

    for s in range(rows):
        live = live_row(rmask_ref, len_ref, s)
        own = prompt_ref[s].astype(F32)
        sums = jnp.zeros((1, LANES), F32)
        for first in firsts:
            sums += down(jnp.where(first[:, 4 * tl + 3 : 4 * tl + 4] == own, first, 0.0))
        count = jnp.maximum(sums[:, 4 * tl : 4 * tl + 1], 1.0)
        total = sums[:, 4 * tl + 1 : 4 * tl + 2]
        mean = total / count
        var = (sums[:, 4 * tl + 2 : 4 * tl + 3] - mean * total) / count
        whitened = (adv_ref[s : s + 1, :] - mean) * lax.rsqrt(var + 1.0)

        tops = [stats_ref[j, s : s + 1, :] for j in range(tn)]
        row_max = functools.reduce(jnp.maximum, tops)
        exp_sum = sum(
            stats_ref[j, rows + s : rows + s + 1, :] * jnp.exp(tops[j] - row_max)
            for j in range(tn)
        )
        target = sum(stats_ref[j, 2 * rows + s : 2 * rows + s + 1, :] for j in range(tn))
        logprob = target - (row_max + jnp.log(exp_sum))

        ratio = jnp.exp(jnp.clip(logprob - old_ref[s : s + 1, :], -20.0, 20.0))
        surrogate = jnp.maximum(-whitened * ratio, -whitened * jnp.clip(ratio, 0.8, 1.2))
        surrogate = jnp.where(whitened < 0.0, jnp.minimum(surrogate, -3.0 * whitened), surrogate)
        drift = jnp.clip(refs[s] - logprob, -20.0, 20.0)
        penalty = jnp.clip(jnp.exp(drift) - drift - 1.0, -10.0, 10.0)
        error = values[s] - ret_ref[s : s + 1, :]
        loss_ref[s : s + 1, :] = live * (surrogate + 0.1 * penalty + 0.25 * error * error)


def per_device(
    logits,
    token_ids,
    response_mask,
    lengths,
    prompt_of,
    old_logprob,
    ref_logprob,
    advantages,
    returns,
    critic_hidden,
    value_weight,
):
    rows, tokens, width = logits.shape
    seqs, tl, feat = critic_hidden.shape
    dp, tn = lax.axis_size("dp"), lax.axis_size("tensor")
    dims = (dp, tn, rows, tl)
    if tokens != LANES or width % LANES or 5 * tl > LANES or LANES % tl or tl < 1:
        raise ValueError("unsupported shapes")
    smem = pl.BlockSpec(memory_space=pltpu.SMEM)
    vmem = pl.BlockSpec(memory_space=pltpu.VMEM)
    weight_row = value_weight[None, :]

    hbm = pl.BlockSpec(memory_space=pltpu.HBM)
    send, part = pl.pallas_call(
        functools.partial(pre_kernel, dims),
        name="pre",
        out_shape=(
            jax.ShapeDtypeStruct((dp * tn * rows, LANES), F32),
            jax.ShapeDtypeStruct((rows, LANES), F32),
        ),
        in_specs=[hbm] * 8,
        out_specs=(hbm, vmem),
        scratch_shapes=[
            pltpu.SMEM(lengths.shape, jnp.int32),
            pltpu.SMEM(prompt_of.shape, jnp.int32),
            pltpu.VMEM((seqs * tl, feat), jnp.bfloat16),
            pltpu.VMEM((feat,), jnp.bfloat16),
            pltpu.VMEM((seqs, tl), jnp.bfloat16),
            pltpu.VMEM((rows, LANES), F32),
            pltpu.VMEM((rows, LANES), jnp.int32),
            pltpu.VMEM((rows, LANES), F32),
            pltpu.VMEM((dp * tn * rows, LANES), F32),
            pltpu.VMEM((seqs, LANES), F32),
            pltpu.SemaphoreType.DMA((9,)),
        ],
        compiler_params=pltpu.CompilerParams(vmem_limit_bytes=6 << 20),
        cost_estimate=pl.CostEstimate(
            flops=40_000_000, bytes_accessed=8_000_000, transcendentals=0
        ),
    )(
        *in_hbm(
            lengths, prompt_of, critic_hidden.reshape(seqs * tl, feat), value_weight, ref_logprob,
            returns, response_mask, advantages,
        )
    )
    received = lax.all_to_all(
        send.reshape(dp * tn, rows, LANES), ("dp", "tensor"), 0, 0, tiled=True
    ).reshape(dp * tn * rows, LANES)

    stats = pl.pallas_call(
        stats_kernel,
        name="stats",
        out_shape=jax.ShapeDtypeStruct((4 * rows, LANES), F32),
        in_specs=[hbm, vmem, hbm],
        out_specs=vmem,
        scratch_shapes=[
            pltpu.VMEM(logits.shape, logits.dtype),
            pltpu.VMEM((rows, tokens), jnp.int32),
            pltpu.VMEM((rows, LANES, LANES), jnp.int32),
            pltpu.VMEM((LANES, LANES), F32),
            pltpu.VMEM((LANES, LANES), F32),
            pltpu.VMEM((LANES, LANES), F32),
            pltpu.SemaphoreType.DMA((rows, 4)),
            pltpu.SemaphoreType.DMA,
        ],
        compiler_params=pltpu.CompilerParams(vmem_limit_bytes=8 << 20),
        cost_estimate=pl.CostEstimate(
            flops=8 * logits.size, bytes_accessed=2 * logits.size, transcendentals=logits.size
        ),
    )(*in_hbm(token_ids), part, *in_hbm(logits))
    gathered = lax.all_gather(stats, "tensor")

    return pl.pallas_call(
        functools.partial(post_kernel, dims),
        name="post",
        compiler_params=pltpu.CompilerParams(vmem_limit_bytes=6 << 20),
        out_shape=(
            jax.ShapeDtypeStruct((rows, tokens), F32),
            jax.ShapeDtypeStruct((seqs, tl, feat), jnp.bfloat16),
        ),
        in_specs=[smem, smem] + [vmem] * 7,
        out_specs=(vmem, vmem),
    )(
        lengths, prompt_of, received, gathered, weight_row, old_logprob, advantages, returns,
        response_mask,
    )


def solution(mesh):
    in_specs = (
        P("dp", None, "tensor"),
        P("dp", None),
        P("dp", None),
        P("dp"),
        P("dp"),
        P("dp", None),
        P(None, "dp"),
        P("dp", None),
        P("dp", None),
        P(None, "dp", "tensor"),
        P("tensor"),
    )
    out_specs = (P("dp", None), P(None, "dp", "tensor"))
    return jax.shard_map(
        per_device, mesh=mesh, in_specs=in_specs, out_specs=out_specs, check_vma=False
    )
```

```python
import functools

import jax
import jax.numpy as jnp
from jax import lax
from jax.experimental import pallas as pl
from jax.experimental.pallas import tpu as pltpu
from jax.sharding import PartitionSpec as P

LANES = 128
F32 = jnp.float32


def fold(x, period):
    shift = LANES // 2
    while shift >= period:
        x = x + pltpu.roll(x, shift, 1)
        shift //= 2
    return x


def in_hbm(*arrays):
    return [pltpu.with_memory_space_constraint(x, pltpu.HBM) for x in arrays]


def live_row(rmask_ref, len_ref, s):
    position = lax.broadcasted_iota(jnp.int32, (1, LANES), 1)
    return jnp.where(position < len_ref[s], rmask_ref[s : s + 1, :], 0).astype(F32)


def group_grid(dp, tl):
    group = lax.broadcasted_iota(jnp.int32, (dp, LANES), 0)
    lane = lax.broadcasted_iota(jnp.int32, (dp, LANES), 1)
    return group, lane, lane // tl


def is_early():
    return lax.axis_index("dp") == 0


def lane_sums(wide):
    total = wide[:, 0:LANES]
    whole = wide.shape[1] // LANES
    for c in range(1, whole):
        total = total + wide[:, c * LANES : (c + 1) * LANES]
    left = wide.shape[1] - whole * LANES
    if left:
        pad = jnp.zeros((wide.shape[0], LANES - left), F32)
        total = total + jnp.concatenate([wide[:, whole * LANES :], pad], axis=1)
    return total


def pre_kernel(
    dims, len_hbm, prompt_hbm, critic_hbm, w_hbm, refl_hbm, ret_hbm, rmask_hbm, adv_hbm,
    ids_hbm, logits_hbm,
    send_hbm, stats_ref,
    len_ref, prompt_ref, critic_ref, w_ref, reflp_ref, ret_ref, rmask_ref, adv_ref, send_ref,
    wide_ref, sems, *scratch,
):
    dp, tn, rows, tl = dims
    pairs = (
        (w_hbm, w_ref), (critic_hbm, critic_ref), (rmask_hbm, rmask_ref), (adv_hbm, adv_ref),
        (ret_hbm, ret_ref), (refl_hbm, reflp_ref), (len_hbm, len_ref), (prompt_hbm, prompt_ref),
    )
    copies = [pltpu.make_async_copy(a, b, sems.at[k]) for k, (a, b) in enumerate(pairs)]
    for copy in copies:
        copy.start()
    for copy in copies[2:]:
        copy.wait()
    wide_ref[:, 0:tl] = reflp_ref[...].astype(F32)
    group, lane, slot = group_grid(dp, tl)
    blocks = []
    for s in range(rows):
        live = live_row(rmask_ref, len_ref, s)
        adv = adv_ref[s : s + 1, :]
        gain = live * adv
        refs = pltpu.roll(wide_ref[pl.ds(s, dp, stride=rows), :], tl, 1)
        rets = jnp.where(slot == group, jnp.broadcast_to(ret_ref[s : s + 1, :], (dp, LANES)), 0.0)
        lives = jnp.where(slot == group, jnp.broadcast_to(live, (dp, LANES)), 0.0)
        block = jnp.where(slot == 1, refs, 0.0)
        block = jnp.where(slot == 2, fold(rets, tl), block)
        block = jnp.where(slot == 3, fold(lives, tl), block)
        block = jnp.where(lane == 4 * tl, jnp.sum(live, axis=1, keepdims=True), block)
        block = jnp.where(lane == 4 * tl + 1, jnp.sum(gain, axis=1, keepdims=True), block)
        block = jnp.where(lane == 4 * tl + 2, jnp.sum(gain * adv, axis=1, keepdims=True), block)
        block = jnp.where(lane == 4 * tl + 3, prompt_ref[s].astype(F32), block)
        blocks.append(block)
    for copy in copies[:2]:
        copy.wait()
    weights = w_ref[...][None, :].astype(F32)
    flat = []
    for h in range(rows):
        wide = critic_ref[h * LANES : (h + 1) * LANES, :].astype(F32) * weights
        flat.append(jnp.sum(jnp.transpose(lane_sums(wide)), axis=0, keepdims=True))
    for h in range(rows):
        stats_ref[3 * rows + h : 3 * rows + h + 1, :] = flat[h]
    for s in range(rows):
        value = jnp.zeros((dp, LANES), F32)
        for h in range(rows):
            line = jnp.broadcast_to(flat[h], (dp, LANES))
            value = jnp.where((h * LANES + lane) // tl == group * rows + s, line, value)
        block = jnp.where(slot == 0, fold(value, tl), blocks[s])
        for j in range(tn):
            send_ref[pl.ds(j * rows + s, dp, stride=tn * rows), :] = block
    out = pltpu.make_async_copy(send_ref, send_hbm, sems.at[len(pairs)])
    out.start()

    @pl.when(is_early())
    def _():
        run_stats(ids_hbm, logits_hbm, stats_ref, *scratch)

    out.wait()


def run_stats(
    ids_hbm, logits_hbm, out_ref,
    logits_ref, ids_ref, ids_smem, here_ref, top_ref, sum_ref, hit_ref, sems, ids_sems,
):
    rows, tokens, width = logits_ref.shape
    chunks = width // LANES
    steps = sems.shape[1]
    step = tokens // steps
    blocks = [(s, k) for s in range(rows) for k in range(steps)]
    copies = [
        pltpu.make_async_copy(
            logits_hbm.at[s, pl.ds(k * step, step)],
            logits_ref.at[s, pl.ds(k * step, step)],
            sems.at[s, k],
        )
        for s, k in blocks
    ]
    ids_copies = [
        pltpu.make_async_copy(ids_hbm, ids_ref, ids_sems.at[0]),
        pltpu.make_async_copy(ids_hbm, ids_smem, ids_sems.at[1]),
    ]
    for copy in ids_copies + copies:
        copy.start()
    start = lax.axis_index("tensor") * width
    lane = lax.broadcasted_iota(jnp.int32, (tokens, LANES), 1)
    for copy in ids_copies:
        copy.wait()
    for s in range(rows):
        ids = jnp.broadcast_to(ids_ref[s : s + 1, :].astype(F32), (LANES, tokens))
        shifted = jnp.transpose(ids).astype(jnp.int32) - start
        here = (lane == (shifted & (LANES - 1))) & (shifted >= 0) & (shifted < width)
        here_ref[s] = here.astype(F32)

    def part_of(n, c):
        s, k = blocks[n]
        return logits_ref[s, k * step : (k + 1) * step, c * LANES : (c + 1) * LANES]

    def shift_of(n):
        copies[n].wait()
        return jnp.max(part_of(n, 0).astype(F32), axis=1, keepdims=True)

    over_lanes = (((1,), (1,)), ((), ()))
    ones = jnp.ones((16, LANES), jnp.bfloat16)

    def sum_row(s):
        return jnp.sum(jnp.transpose(sum_ref[s]), axis=0, keepdims=True)

    def top_row(s):
        return lax.dot_general(
            ones * (1.0 / LANES), top_ref[s], over_lanes, preferred_element_type=F32
        )[0:1, :]

    row8 = lax.broadcasted_iota(jnp.int32, (8, LANES), 0)
    worst = jnp.zeros((8, LANES), F32)
    top = shift_of(0)
    for n, (s, k) in enumerate(blocks):
        later = shift_of(n + 1) if n + 1 < len(blocks) else None
        at = slice(k * step, (k + 1) * step)
        total = jnp.zeros((step, LANES), F32)
        for c in range(chunks):
            total = total + jnp.exp(part_of(n, c).astype(F32) - top)
        top_ref[s, at, :] = jnp.broadcast_to(top, (step, LANES)).astype(jnp.bfloat16)
        sum_ref[s, at, :] = total
        for q in range(step // 8):
            worst = jnp.maximum(worst, total[q * 8 : (q + 1) * 8, :])
            first = k * step + q * 8
            hit = jnp.zeros((8, LANES), F32)
            for r in range(8):
                chunk = jnp.clip((ids_smem[s, first + r] - start) >> 7, 0, chunks - 1)
                cols = pl.ds(pl.multiple_of(chunk * LANES, LANES), LANES)
                x = logits_ref[s, first : first + 8, cols].astype(F32)
                hit = jnp.where(row8 == r, x, hit)
            here = here_ref[s, first : first + 8, :] > 0.0
            hit_ref[s, first : first + 8, :] = jnp.where(here, hit, 0.0)
        top = later
        if k == steps - 1:
            hits = lax.dot_general(
                ones, hit_ref[s].astype(jnp.bfloat16), over_lanes, preferred_element_type=F32
            )
            out_ref[s : s + 1, :] = top_row(s)
            out_ref[rows + s : rows + s + 1, :] = sum_row(s)
            out_ref[2 * rows + s : 2 * rows + s + 1, :] = hits[0:1, :]

    @pl.when(jnp.logical_not(jnp.max(worst) < 1e30))
    def _():
        for s in range(rows):

            def again(k, carry, s=s):
                at = pl.ds(pl.multiple_of(k * 32, 32), 32)
                top = logits_ref[s, at, 0:LANES]
                for c in range(1, chunks):
                    top = jnp.maximum(top, logits_ref[s, at, c * LANES : (c + 1) * LANES])
                top = jnp.max(top.astype(F32), axis=1, keepdims=True)
                total = jnp.zeros((32, LANES), F32)
                for c in range(chunks):
                    x = logits_ref[s, at, c * LANES : (c + 1) * LANES].astype(F32)
                    total = total + jnp.exp(x - top)
                top_ref[s, at, :] = jnp.broadcast_to(top, (32, LANES)).astype(jnp.bfloat16)
                sum_ref[s, at, :] = total
                return carry

            lax.fori_loop(0, tokens // 32, again, 0)
            out_ref[s : s + 1, :] = top_row(s)
            out_ref[rows + s : rows + s + 1, :] = sum_row(s)


def stats_kernel(ids_hbm, early_ref, logits_hbm, out_ref, *scratch):
    out_ref[...] = early_ref[...]

    @pl.when(jnp.logical_not(is_early()))
    def _():
        run_stats(ids_hbm, logits_hbm, out_ref, *scratch)


def merge_kernel(dims, old_ref, *refs):
    dp, tn, rows, tl = dims
    stats, (logprob_ref, ratio_ref, tile_ref) = refs[:tn], refs[tn:]
    seqs = dp * rows
    tops = [stat[0:rows, :] for stat in stats]
    row_max = functools.reduce(jnp.maximum, tops)
    exp_sum = sum(
        stat[rows : 2 * rows, :] * jnp.exp(top - row_max) for stat, top in zip(stats, tops)
    )
    target = sum(stat[2 * rows : 3 * rows, :] for stat in stats)
    logprob = target - (row_max + jnp.log(exp_sum))
    logprob_ref[...] = logprob
    ratio_ref[...] = jnp.exp(jnp.clip(logprob - old_ref[...], -20.0, 20.0))

    order = lax.broadcasted_iota(jnp.int32, (seqs, LANES), 0)
    seq = (order % dp) * rows + order // dp
    lane = lax.broadcasted_iota(jnp.int32, (seqs, LANES), 1)
    tile = jnp.zeros((seqs, LANES), F32)
    for h in range(rows):
        line = sum(stat[3 * rows + h : 3 * rows + h + 1, :] for stat in stats)
        here = (h * LANES + lane) // tl == seq
        tile = jnp.where(here, jnp.broadcast_to(line, (seqs, LANES)), tile)
    tile_ref[...] = jnp.transpose(fold(tile, tl))[0:tl, :]


def post_kernel(
    dims, len_ref, prompt_ref, recv_ref, w_ref, adv_ref, ret_ref, rmask_ref,
    logprob_ref, ratio_ref, tile_ref,
    loss_hbm, grad_hbm, loss_ref, grad_ref, sems,
):
    dp, tn, rows, tl = dims
    seqs = dp * rows
    group, lane, slot = group_grid(dp, tl)
    parts = [
        [recv_ref[pl.ds(j * rows + s, dp, stride=tn * rows), :] for j in range(tn)]
        for s in range(rows)
    ]
    firsts = [part[0] for part in parts]

    columns = jnp.transpose(jnp.concatenate(firsts, axis=0))
    coeff = (
        32.0 * columns[3 * tl : 4 * tl, :] * (tile_ref[...] - columns[2 * tl : 3 * tl, :])
    )
    weights = w_ref[...][None, :].astype(F32)
    pieces = sems.shape[0] - 1
    piece = seqs // pieces
    copies = []
    for k in range(pieces):
        for b in range(k * piece, (k + 1) * piece):
            at = (b % rows) * dp + b // rows
            grad_ref[b] = (coeff[:, at : at + 1] * weights).astype(grad_ref.dtype)
        at = pl.ds(k * piece, piece)
        copies.append(pltpu.make_async_copy(grad_ref.at[at], grad_hbm.at[at], sems.at[k]))
        copies[-1].start()

    def row_of(x, k):
        apart = pltpu.roll(x, 0, 1, stride=tl, stride_axis=0)
        row = jnp.sum(jnp.where(slot == (group + k) % dp, apart, 0.0), axis=0, keepdims=True)
        return pltpu.roll(row, LANES - k * tl, 1) if k else row

    for s in range(rows):
        value_pred = row_of(sum(parts[s][1:], firsts[s]), 0)
        ref_row = row_of(firsts[s], 1)
        own = prompt_ref[s].astype(F32)
        sums = jnp.zeros((1, LANES), F32)
        for first in firsts:
            same = first[:, 4 * tl + 3 : 4 * tl + 4] == own
            sums += jnp.sum(jnp.where(same, first, 0.0), axis=0, keepdims=True)
        count = jnp.maximum(sums[:, 4 * tl : 4 * tl + 1], 1.0)
        total = sums[:, 4 * tl + 1 : 4 * tl + 2]
        mean = total / count
        var = (sums[:, 4 * tl + 2 : 4 * tl + 3] - mean * total) / count
        whitened = (adv_ref[s : s + 1, :] - mean) * lax.rsqrt(var + 1.0)

        ratio = ratio_ref[s : s + 1, :]
        surrogate = jnp.maximum(-whitened * ratio, -whitened * jnp.clip(ratio, 0.8, 1.2))
        surrogate = jnp.where(whitened < 0.0, jnp.minimum(surrogate, -3.0 * whitened), surrogate)
        drift = jnp.clip(ref_row - logprob_ref[s : s + 1, :], -20.0, 20.0)
        penalty = jnp.clip(jnp.exp(drift) - drift - 1.0, -10.0, 10.0)
        error = value_pred - ret_ref[s : s + 1, :]
        live = live_row(rmask_ref, len_ref, s)
        loss_ref[s : s + 1, :] = live * (surrogate + 0.1 * penalty + 0.25 * error * error)
    copies.append(pltpu.make_async_copy(loss_ref, loss_hbm, sems.at[pieces]))
    copies[-1].start()
    for copy in copies:
        copy.wait()


def per_device(
    logits,
    token_ids,
    response_mask,
    lengths,
    prompt_of,
    old_logprob,
    ref_logprob,
    advantages,
    returns,
    critic_hidden,
    value_weight,
):
    rows, tokens, width = logits.shape
    seqs, tl, feat = critic_hidden.shape
    dp, tn = lax.axis_size("dp"), lax.axis_size("tensor")
    dims = (dp, tn, rows, tl)
    if tokens != LANES or width % LANES or 5 * tl > LANES or LANES % tl or tn & (tn - 1):
        raise ValueError("unsupported shapes")
    smem = pl.BlockSpec(memory_space=pltpu.SMEM)
    vmem = pl.BlockSpec(memory_space=pltpu.VMEM)
    hbm = pl.BlockSpec(memory_space=pltpu.HBM)

    def grant(mib):
        return pltpu.CompilerParams(vmem_limit_bytes=mib << 20)

    stats_scratch = [
        pltpu.VMEM(logits.shape, logits.dtype),
        pltpu.VMEM((rows, tokens), jnp.int32),
        pltpu.SMEM((rows, tokens), jnp.int32),
        pltpu.VMEM((rows, tokens, LANES), F32),
        pltpu.VMEM((rows, tokens, LANES), jnp.bfloat16),
        pltpu.VMEM((rows, tokens, LANES), F32),
        pltpu.VMEM((rows, tokens, LANES), F32),
        pltpu.SemaphoreType.DMA((rows, 4)),
        pltpu.SemaphoreType.DMA((2,)),
    ]
    send, early = pl.pallas_call(
        functools.partial(pre_kernel, dims),
        name="pre",
        out_shape=(
            jax.ShapeDtypeStruct((dp * tn * rows, LANES), F32),
            jax.ShapeDtypeStruct((4 * rows, LANES), F32),
        ),
        in_specs=[hbm] * 10,
        out_specs=(hbm, vmem),
        scratch_shapes=[
            pltpu.SMEM(lengths.shape, jnp.int32),
            pltpu.SMEM(prompt_of.shape, jnp.int32),
            pltpu.VMEM((seqs * tl, feat), jnp.bfloat16),
            pltpu.VMEM((feat,), jnp.bfloat16),
            pltpu.VMEM((seqs, tl), jnp.bfloat16),
            pltpu.VMEM((rows, LANES), F32),
            pltpu.VMEM((rows, LANES), jnp.int32),
            pltpu.VMEM((rows, LANES), F32),
            pltpu.VMEM((dp * tn * rows, LANES), F32),
            pltpu.VMEM((seqs, LANES), F32),
            pltpu.SemaphoreType.DMA((9,)),
            *stats_scratch,
        ],
        compiler_params=grant(10),
    )(
        *in_hbm(
            lengths, prompt_of, critic_hidden.reshape(seqs * tl, feat), value_weight, ref_logprob,
            returns, response_mask, advantages, token_ids, logits,
        )
    )
    received = lax.all_to_all(
        send.reshape(dp * tn, rows, LANES), ("dp", "tensor"), 0, 0, tiled=True
    ).reshape(dp * tn * rows, LANES)

    stats = pl.pallas_call(
        stats_kernel,
        name="stats",
        out_shape=jax.ShapeDtypeStruct((4 * rows, LANES), F32),
        in_specs=[hbm, vmem, hbm],
        out_specs=vmem,
        scratch_shapes=stats_scratch,
        compiler_params=grant(8),
        cost_estimate=pl.CostEstimate(
            flops=8 * logits.size, bytes_accessed=2 * logits.size, transcendentals=logits.size
        ),
    )(*in_hbm(token_ids), early, *in_hbm(logits))
    shards = [stats] + [
        lax.ppermute(stats, "tensor", [(t, t ^ k) for t in range(tn)])
        for k in reversed(range(1, tn))
    ]

    merged = pl.pallas_call(
        functools.partial(merge_kernel, dims),
        name="merge",
        out_shape=(
            jax.ShapeDtypeStruct((rows, LANES), F32),
            jax.ShapeDtypeStruct((rows, LANES), F32),
            jax.ShapeDtypeStruct((tl, seqs), F32),
        ),
        in_specs=[vmem] * (1 + tn),
        out_specs=(vmem,) * 3,
        compiler_params=grant(4),
    )(old_logprob, *shards)

    return pl.pallas_call(
        functools.partial(post_kernel, dims),
        name="post",
        out_shape=(
            jax.ShapeDtypeStruct((rows, tokens), F32),
            jax.ShapeDtypeStruct((seqs, tl, feat), jnp.bfloat16),
        ),
        in_specs=[smem, smem] + [vmem] * 8,
        out_specs=(hbm, hbm),
        scratch_shapes=[
            pltpu.VMEM((rows, tokens), F32),
            pltpu.VMEM((seqs, tl, feat), jnp.bfloat16),
            pltpu.SemaphoreType.DMA((5,)),
        ],
        compiler_params=grant(6),
    )(lengths, prompt_of, received, value_weight, advantages, returns, response_mask, *merged)


def solution(mesh):
    in_specs = (
        P("dp", None, "tensor"),
        P("dp", None),
        P("dp", None),
        P("dp"),
        P("dp"),
        P("dp", None),
        P(None, "dp"),
        P("dp", None),
        P("dp", None),
        P(None, "dp", "tensor"),
        P("tensor"),
    )
    out_specs = (P("dp", None), P(None, "dp", "tensor"))
    return jax.shard_map(
        per_device, mesh=mesh, in_specs=in_specs, out_specs=out_specs, check_vma=False
    )
```

```python
import functools

import jax
import jax.numpy as jnp
from jax import lax
from jax.experimental import pallas as pl
from jax.experimental.pallas import tpu as pltpu
from jax.sharding import PartitionSpec as P

LANES = 128
STEPS = 4
F32 = jnp.float32


def fold(x, period):
    shift = LANES // 2
    while shift >= period:
        x = x + pltpu.roll(x, shift, 1)
        shift //= 2
    return x


def in_hbm(*arrays):
    return [pltpu.with_memory_space_constraint(x, pltpu.HBM) for x in arrays]


def live_row(rmask_ref, len_ref, s):
    position = lax.broadcasted_iota(jnp.int32, (1, LANES), 1)
    return jnp.where(position < len_ref[s], rmask_ref[s : s + 1, :], 0).astype(F32)


def group_grid(dp, tl):
    group = lax.broadcasted_iota(jnp.int32, (dp, LANES), 0)
    lane = lax.broadcasted_iota(jnp.int32, (dp, LANES), 1)
    return group, lane, lane // tl


def is_early():
    return lax.axis_index("dp") == 0


def lane_sums(wide):
    total = wide[:, 0:LANES]
    whole = wide.shape[1] // LANES
    for c in range(1, whole):
        total = total + wide[:, c * LANES : (c + 1) * LANES]
    left = wide.shape[1] - whole * LANES
    if left:
        pad = jnp.zeros((wide.shape[0], LANES - left), F32)
        total = total + jnp.concatenate([wide[:, whole * LANES :], pad], axis=1)
    return total


def pre_kernel(
    dims, len_hbm, prompt_hbm, critic_hbm, w_hbm, refl_hbm, ret_hbm, rmask_hbm, adv_hbm,
    ids_hbm, logits_hbm,
    send_hbm, stats_ref, local_ref,
    len_ref, prompt_ref, critic_ref, w_ref, reflp_ref, ret_ref, rmask_ref, adv_ref, send_ref,
    wide_ref, sems, *scratch,
):
    dp, tn, rows, tl = dims
    pairs = (
        (w_hbm, w_ref), (critic_hbm, critic_ref), (rmask_hbm, rmask_ref), (adv_hbm, adv_ref),
        (ret_hbm, ret_ref), (refl_hbm, reflp_ref), (len_hbm, len_ref), (prompt_hbm, prompt_ref),
    )
    copies = [pltpu.make_async_copy(a, b, sems.at[k]) for k, (a, b) in enumerate(pairs)]
    for copy in copies:
        copy.start()
    for copy in copies[2:]:
        copy.wait()
    wide_ref[:, 0:tl] = reflp_ref[...].astype(F32)
    group, lane, slot = group_grid(dp, tl)
    place = (lane - group * (rows * tl)) & (LANES - 1)
    spot = place // tl
    blocks = []
    for s in range(rows):
        live = live_row(rmask_ref, len_ref, s)
        adv = adv_ref[s : s + 1, :]
        gain = live * adv
        prompt = prompt_ref[s].astype(F32)
        local_ref[s : s + 1, :] = live
        local_ref[rows + s : rows + s + 1, :] = jnp.zeros((1, LANES), F32) + prompt
        local_ref[2 * rows + s : 2 * rows + s + 1, :] = adv
        local_ref[3 * rows + s : 3 * rows + s + 1, :] = ret_ref[s : s + 1, :]
        refs = jnp.where(slot == 0, wide_ref[pl.ds(s, dp, stride=rows), :], 0.0)
        rets = jnp.where(slot == group, jnp.broadcast_to(ret_ref[s : s + 1, :], (dp, LANES)), 0.0)
        lives = jnp.where(slot == group, jnp.broadcast_to(live, (dp, LANES)), 0.0)
        block = jnp.where(spot == rows, fold(refs, tl), 0.0)
        block = jnp.where(spot == rows + 1, fold(rets, tl), block)
        block = jnp.where(spot == rows + 2, fold(lives, tl), block)
        last = (rows + 3) * tl
        block = jnp.where(place == last, jnp.sum(live, axis=1, keepdims=True), block)
        block = jnp.where(place == last + 1, jnp.sum(gain, axis=1, keepdims=True), block)
        block = jnp.where(place == last + 2, jnp.sum(gain * adv, axis=1, keepdims=True), block)
        block = jnp.where(place == last + 3, prompt, block)
        blocks.append(block)
    for copy in copies[:2]:
        copy.wait()
    weights = w_ref[...][None, :].astype(F32)
    flat = []
    for h in range(rows):
        wide = critic_ref[h * LANES : (h + 1) * LANES, :].astype(F32) * weights
        flat.append(jnp.sum(jnp.transpose(lane_sums(wide)), axis=0, keepdims=True))
    for h in range(rows):
        stats_ref[3 * rows + h : 3 * rows + h + 1, :] = flat[h]
    for s in range(rows):
        block = blocks[s]
        for h in range(rows):
            line = jnp.broadcast_to(flat[h], (dp, LANES))
            block = jnp.where((h * LANES + lane) // tl == group * rows + s, line, block)
        for j in range(tn):
            send_ref[pl.ds(j * rows + s, dp, stride=tn * rows), :] = block
    out = pltpu.make_async_copy(send_ref, send_hbm, sems.at[sems.shape[0] - 1])
    out.start()

    @pl.when(is_early())
    def _():
        run_stats(ids_hbm, logits_hbm, stats_ref, *scratch, sems)

    out.wait()


def run_stats(
    ids_hbm, logits_hbm, out_ref,
    logits_ref, ids_ref, ids_smem, here_ref, top_ref, sum_ref, hit_ref, sems,
):
    rows, tokens, width = logits_ref.shape
    chunks = width // LANES
    steps = STEPS
    step = tokens // steps
    blocks = [(s, k) for s in range(rows) for k in range(steps)]
    copies = [
        pltpu.make_async_copy(
            logits_hbm.at[s, pl.ds(k * step, step)],
            logits_ref.at[s, pl.ds(k * step, step)],
            sems.at[s * steps + k],
        )
        for s, k in blocks
    ]
    ids_copies = [
        pltpu.make_async_copy(ids_hbm, ids_ref, sems.at[rows * steps]),
        pltpu.make_async_copy(ids_hbm, ids_smem, sems.at[rows * steps + 1]),
    ]
    for copy in ids_copies + copies:
        copy.start()
    start = lax.axis_index("tensor") * width
    lane = lax.broadcasted_iota(jnp.int32, (tokens, LANES), 1)
    for copy in ids_copies:
        copy.wait()
    for s in range(rows):
        ids = jnp.broadcast_to(ids_ref[s : s + 1, :].astype(F32), (LANES, tokens))
        shifted = jnp.transpose(ids).astype(jnp.int32) - start
        here = (lane == (shifted & (LANES - 1))) & (shifted >= 0) & (shifted < width)
        here_ref[s] = here.astype(F32)

    def part_of(n, c):
        s, k = blocks[n]
        return logits_ref[s, k * step : (k + 1) * step, c * LANES : (c + 1) * LANES]

    def shift_of(n):
        copies[n].wait()
        return jnp.max(part_of(n, 0).astype(F32), axis=1, keepdims=True)

    over_lanes = (((1,), (1,)), ((), ()))
    ones = jnp.ones((16, LANES), jnp.bfloat16)

    def sum_row(s):
        return jnp.sum(jnp.transpose(sum_ref[s]), axis=0, keepdims=True)

    def top_row(s):
        return lax.dot_general(
            ones * (1.0 / LANES), top_ref[s], over_lanes, preferred_element_type=F32
        )[0:1, :]

    row8 = lax.broadcasted_iota(jnp.int32, (8, LANES), 0)
    worst = jnp.zeros((8, LANES), F32)
    top = shift_of(0)
    for n, (s, k) in enumerate(blocks):
        later = shift_of(n + 1) if n + 1 < len(blocks) else None
        at = slice(k * step, (k + 1) * step)
        total = jnp.zeros((step, LANES), F32)
        for c in range(chunks):
            total = total + jnp.exp(part_of(n, c).astype(F32) - top)
        top_ref[s, at, :] = jnp.broadcast_to(top, (step, LANES)).astype(jnp.bfloat16)
        sum_ref[s, at, :] = total
        for q in range(step // 8):
            worst = jnp.maximum(worst, total[q * 8 : (q + 1) * 8, :])
            first = k * step + q * 8
            hit = jnp.zeros((8, LANES), F32)
            for r in range(8):
                chunk = jnp.clip((ids_smem[s, first + r] - start) >> 7, 0, chunks - 1)
                cols = pl.ds(pl.multiple_of(chunk * LANES, LANES), LANES)
                x = logits_ref[s, first : first + 8, cols].astype(F32)
                hit = jnp.where(row8 == r, x, hit)
            here = here_ref[s, first : first + 8, :] > 0.0
            hit_ref[s, first : first + 8, :] = jnp.where(here, hit, 0.0)
        top = later
        if k == steps - 1:
            hits = lax.dot_general(
                ones, hit_ref[s].astype(jnp.bfloat16), over_lanes, preferred_element_type=F32
            )
            out_ref[s : s + 1, :] = top_row(s)
            out_ref[rows + s : rows + s + 1, :] = sum_row(s)
            out_ref[2 * rows + s : 2 * rows + s + 1, :] = hits[0:1, :]

    @pl.when(jnp.logical_not(jnp.max(worst) < 1e30))
    def _():
        for s in range(rows):

            def again(k, carry, s=s):
                at = pl.ds(pl.multiple_of(k * 32, 32), 32)
                top = logits_ref[s, at, 0:LANES]
                for c in range(1, chunks):
                    top = jnp.maximum(top, logits_ref[s, at, c * LANES : (c + 1) * LANES])
                top = jnp.max(top.astype(F32), axis=1, keepdims=True)
                total = jnp.zeros((32, LANES), F32)
                for c in range(chunks):
                    x = logits_ref[s, at, c * LANES : (c + 1) * LANES].astype(F32)
                    total = total + jnp.exp(x - top)
                top_ref[s, at, :] = jnp.broadcast_to(top, (32, LANES)).astype(jnp.bfloat16)
                sum_ref[s, at, :] = total
                return carry

            lax.fori_loop(0, tokens // 32, again, 0)
            out_ref[s : s + 1, :] = top_row(s)
            out_ref[rows + s : rows + s + 1, :] = sum_row(s)


def stats_kernel(ids_hbm, early_ref, logits_hbm, out_ref, *scratch):
    out_ref[...] = early_ref[...]

    @pl.when(jnp.logical_not(is_early()))
    def _():
        run_stats(ids_hbm, logits_hbm, out_ref, *scratch)


def merge_kernel(dims, old_ref, *refs):
    dp, tn, rows, tl = dims
    stats, (logprob_ref, ratio_ref, tile_ref) = refs[:tn], refs[tn:]
    seqs = dp * rows
    tops = [stat[0:rows, :] for stat in stats]
    row_max = functools.reduce(jnp.maximum, tops)
    exp_sum = sum(
        stat[rows : 2 * rows, :] * jnp.exp(top - row_max) for stat, top in zip(stats, tops)
    )
    target = sum(stat[2 * rows : 3 * rows, :] for stat in stats)
    logprob = target - (row_max + jnp.log(exp_sum))
    logprob_ref[...] = logprob
    ratio_ref[...] = jnp.exp(jnp.clip(logprob - old_ref[...], -20.0, 20.0))

    order = lax.broadcasted_iota(jnp.int32, (seqs, LANES), 0)
    seq = (order % dp) * rows + order // dp
    lane = lax.broadcasted_iota(jnp.int32, (seqs, LANES), 1)
    tile = jnp.zeros((seqs, LANES), F32)
    for h in range(rows):
        line = sum(stat[3 * rows + h : 3 * rows + h + 1, :] for stat in stats)
        here = (h * LANES + lane) // tl == seq
        tile = jnp.where(here, jnp.broadcast_to(line, (seqs, LANES)), tile)
    tile_ref[...] = jnp.transpose(fold(tile, tl))[0:tl, :]


def post_kernel(
    dims, recv_ref, w_ref, local_ref, logprob_ref, ratio_ref, tile_ref,
    loss_hbm, grad_hbm, loss_ref, grad_ref, sems,
):
    dp, tn, rows, tl = dims
    seqs = dp * rows
    group, lane, slot = group_grid(dp, tl)
    parts = [
        [recv_ref[pl.ds(j * rows + s, dp, stride=tn * rows), :] for j in range(tn)]
        for s in range(rows)
    ]
    back = LANES - (lax.axis_index("dp") * (rows * tl)) % LANES
    firsts = [pltpu.roll(part[0], back, 1) for part in parts]
    every = [pltpu.roll(sum(part[1:], part[0]), back, 1) for part in parts]

    def row_of(x, k):
        apart = pltpu.roll(x, 0, 1, stride=tl, stride_axis=0)
        row = jnp.sum(jnp.where(slot == (group + k) % dp, apart, 0.0), axis=0, keepdims=True)
        return pltpu.roll(row, LANES - k * tl, 1) if k else row

    spot = (rows + 3) * tl
    prompts = [first[:, spot + 3 : spot + 4] for first in firsts]

    columns = jnp.transpose(jnp.concatenate(firsts, axis=0))
    at = (rows + 1) * tl
    coeff = (
        32.0 * columns[at + tl : at + 2 * tl, :] * (tile_ref[...] - columns[at : at + tl, :])
    )
    weights = w_ref[...][None, :].astype(F32)
    pieces = sems.shape[0] - 1
    piece = seqs // pieces
    copies = []
    for k in range(pieces):
        for b in range(k * piece, (k + 1) * piece):
            at = (b % rows) * dp + b // rows
            grad_ref[b] = (coeff[:, at : at + 1] * weights).astype(grad_ref.dtype)
        at = pl.ds(k * piece, piece)
        copies.append(pltpu.make_async_copy(grad_ref.at[at], grad_hbm.at[at], sems.at[k]))
        copies[-1].start()

    for s in range(rows):
        value_pred = row_of(every[s], s)
        ref_row = row_of(firsts[s], rows)
        own = local_ref[rows + s : rows + s + 1, 0:1]
        sums = jnp.zeros((1, LANES), F32)
        for first, prompt in zip(firsts, prompts):
            sums += jnp.sum(jnp.where(prompt == own, first, 0.0), axis=0, keepdims=True)
        count = jnp.maximum(sums, 1.0)
        total = pltpu.roll(sums, LANES - 1, 1)
        square = pltpu.roll(sums, LANES - 2, 1)
        mean = total / count
        scale = lax.rsqrt((square - mean * total) / count + 1.0)
        adv = local_ref[2 * rows + s : 2 * rows + s + 1, :]
        whitened = (adv - mean[:, spot : spot + 1]) * scale[:, spot : spot + 1]

        ratio = ratio_ref[s : s + 1, :]
        surrogate = jnp.maximum(-whitened * ratio, -whitened * jnp.clip(ratio, 0.8, 1.2))
        surrogate = jnp.where(whitened < 0.0, jnp.minimum(surrogate, -3.0 * whitened), surrogate)
        drift = jnp.clip(ref_row - logprob_ref[s : s + 1, :], -20.0, 20.0)
        penalty = jnp.clip(jnp.exp(drift) - drift - 1.0, -10.0, 10.0)
        error = value_pred - local_ref[3 * rows + s : 3 * rows + s + 1, :]
        live = local_ref[s : s + 1, :]
        loss_ref[s : s + 1, :] = live * (surrogate + 0.1 * penalty + 0.25 * error * error)
    copies.append(pltpu.make_async_copy(loss_ref, loss_hbm, sems.at[pieces]))
    copies[-1].start()
    for copy in copies:
        copy.wait()


def per_device(
    logits,
    token_ids,
    response_mask,
    lengths,
    prompt_of,
    old_logprob,
    ref_logprob,
    advantages,
    returns,
    critic_hidden,
    value_weight,
):
    rows, tokens, width = logits.shape
    seqs, tl, feat = critic_hidden.shape
    dp, tn = lax.axis_size("dp"), lax.axis_size("tensor")
    dims = (dp, tn, rows, tl)
    if tokens != LANES or width % LANES or (rows + 3) * tl + 4 > LANES or LANES % tl or tn & (tn - 1):
        raise ValueError("unsupported shapes")
    vmem = pl.BlockSpec(memory_space=pltpu.VMEM)
    hbm = pl.BlockSpec(memory_space=pltpu.HBM)

    def grant(mib):
        return pltpu.CompilerParams(vmem_limit_bytes=mib << 20)

    stats_scratch = [
        pltpu.VMEM(logits.shape, logits.dtype),
        pltpu.VMEM((rows, tokens), jnp.int32),
        pltpu.SMEM((rows, tokens), jnp.int32),
        pltpu.VMEM((rows, tokens, LANES), F32),
        pltpu.VMEM((rows, tokens, LANES), jnp.bfloat16),
        pltpu.VMEM((rows, tokens, LANES), F32),
        pltpu.VMEM((rows, tokens, LANES), F32),
    ]
    copies = rows * STEPS + 2
    send, early, local = pl.pallas_call(
        functools.partial(pre_kernel, dims),
        name="pre",
        out_shape=(
            jax.ShapeDtypeStruct((dp * tn * rows, LANES), F32),
            jax.ShapeDtypeStruct((4 * rows, LANES), F32),
            jax.ShapeDtypeStruct((4 * rows, LANES), F32),
        ),
        in_specs=[hbm] * 10,
        out_specs=(hbm, vmem, vmem),
        scratch_shapes=[
            pltpu.SMEM(lengths.shape, jnp.int32),
            pltpu.SMEM(prompt_of.shape, jnp.int32),
            pltpu.VMEM((seqs * tl, feat), jnp.bfloat16),
            pltpu.VMEM((feat,), jnp.bfloat16),
            pltpu.VMEM((seqs, tl), jnp.bfloat16),
            pltpu.VMEM((rows, LANES), F32),
            pltpu.VMEM((rows, LANES), jnp.int32),
            pltpu.VMEM((rows, LANES), F32),
            pltpu.VMEM((dp * tn * rows, LANES), F32),
            pltpu.VMEM((seqs, LANES), F32),
            pltpu.SemaphoreType.DMA((max(copies, 8) + 1,)),
            *stats_scratch,
        ],
        compiler_params=grant(10),
    )(
        *in_hbm(
            lengths, prompt_of, critic_hidden.reshape(seqs * tl, feat), value_weight, ref_logprob,
            returns, response_mask, advantages, token_ids, logits,
        )
    )
    received = lax.all_to_all(
        send.reshape(dp * tn, rows, LANES), ("dp", "tensor"), 0, 0, tiled=True
    ).reshape(dp * tn * rows, LANES)

    stats = pl.pallas_call(
        stats_kernel,
        name="stats",
        out_shape=jax.ShapeDtypeStruct((4 * rows, LANES), F32),
        in_specs=[hbm, vmem, hbm],
        out_specs=vmem,
        scratch_shapes=[*stats_scratch, pltpu.SemaphoreType.DMA((copies,))],
        compiler_params=grant(8),
        cost_estimate=pl.CostEstimate(
            flops=8 * logits.size, bytes_accessed=2 * logits.size, transcendentals=logits.size
        ),
    )(*in_hbm(token_ids), early, *in_hbm(logits))
    shards = [stats] + [
        lax.ppermute(stats, "tensor", [(t, t ^ k) for t in range(tn)])
        for k in reversed(range(1, tn))
    ]

    merged = pl.pallas_call(
        functools.partial(merge_kernel, dims),
        name="merge",
        out_shape=(
            jax.ShapeDtypeStruct((rows, LANES), F32),
            jax.ShapeDtypeStruct((rows, LANES), F32),
            jax.ShapeDtypeStruct((tl, seqs), F32),
        ),
        in_specs=[vmem] * (1 + tn),
        out_specs=(vmem,) * 3,
        compiler_params=grant(4),
    )(old_logprob, *shards)

    return pl.pallas_call(
        functools.partial(post_kernel, dims),
        name="post",
        out_shape=(
            jax.ShapeDtypeStruct((rows, tokens), F32),
            jax.ShapeDtypeStruct((seqs, tl, feat), jnp.bfloat16),
        ),
        in_specs=[vmem] * 6,
        out_specs=(hbm, hbm),
        scratch_shapes=[
            pltpu.VMEM((rows, tokens), F32),
            pltpu.VMEM((seqs, tl, feat), jnp.bfloat16),
            pltpu.SemaphoreType.DMA((3,)),
        ],
        compiler_params=grant(6),
    )(received, value_weight, local, *merged)


def solution(mesh):
    in_specs = (
        P("dp", None, "tensor"),
        P("dp", None),
        P("dp", None),
        P("dp"),
        P("dp"),
        P("dp", None),
        P(None, "dp"),
        P("dp", None),
        P("dp", None),
        P(None, "dp", "tensor"),
        P("tensor"),
    )
    out_specs = (P("dp", None), P(None, "dp", "tensor"))
    return jax.shard_map(
        per_device, mesh=mesh, in_specs=in_specs, out_specs=out_specs, check_vma=False
    )
```

```python
import functools

import jax
import jax.numpy as jnp
from jax import lax
from jax.experimental import pallas as pl
from jax.experimental.pallas import tpu as pltpu
from jax.sharding import PartitionSpec as P

LANES = 128
STEPS = 4
F32 = jnp.float32


def fold(x, period):
    shift = LANES // 2
    while shift >= period:
        x = x + pltpu.roll(x, shift, 1)
        shift //= 2
    return x


def in_hbm(*arrays):
    return [pltpu.with_memory_space_constraint(x, pltpu.HBM) for x in arrays]


def live_row(rmask_ref, len_ref, s):
    position = lax.broadcasted_iota(jnp.int32, (1, LANES), 1)
    return jnp.where(position < len_ref[s], rmask_ref[s : s + 1, :], 0).astype(F32)


def group_grid(dp, tl):
    group = lax.broadcasted_iota(jnp.int32, (dp, LANES), 0)
    lane = lax.broadcasted_iota(jnp.int32, (dp, LANES), 1)
    return group, lane, lane // tl


def is_early():
    return lax.axis_index("dp") == 0


def lane_sums(wide):
    total = wide[:, 0:LANES]
    whole = wide.shape[1] // LANES
    for c in range(1, whole):
        total = total + wide[:, c * LANES : (c + 1) * LANES]
    left = wide.shape[1] - whole * LANES
    if left:
        pad = jnp.zeros((wide.shape[0], LANES - left), F32)
        total = total + jnp.concatenate([wide[:, whole * LANES :], pad], axis=1)
    return total


def pre_kernel(
    dims, len_hbm, prompt_hbm, critic_hbm, w_hbm, refl_hbm, ret_hbm, rmask_hbm, adv_hbm,
    ids_hbm, logits_hbm,
    send_hbm, stats_ref, local_ref,
    len_ref, prompt_ref, critic_ref, w_ref, reflp_ref, ret_ref, rmask_ref, adv_ref, send_ref,
    wide_ref, sems, *scratch,
):
    dp, tn, rows, tl = dims
    pairs = (
        (w_hbm, w_ref), (critic_hbm, critic_ref), (rmask_hbm, rmask_ref), (adv_hbm, adv_ref),
        (ret_hbm, ret_ref), (refl_hbm, reflp_ref), (len_hbm, len_ref), (prompt_hbm, prompt_ref),
    )
    copies = [pltpu.make_async_copy(a, b, sems.at[k]) for k, (a, b) in enumerate(pairs)]
    for copy in copies[::-1]:
        copy.start()
    for copy in copies[2:]:
        copy.wait()
    wide_ref[:, 0:tl] = reflp_ref[...].astype(F32)
    group, lane, slot = group_grid(dp, tl)
    place = (lane - group * (rows * tl)) & (LANES - 1)
    spot = place // tl
    blocks = []
    for s in range(rows):
        live = live_row(rmask_ref, len_ref, s)
        adv = adv_ref[s : s + 1, :]
        gain = live * adv
        prompt = prompt_ref[s].astype(F32)
        local_ref[s : s + 1, :] = live
        local_ref[rows + s : rows + s + 1, :] = jnp.zeros((1, LANES), F32) + prompt
        local_ref[2 * rows + s : 2 * rows + s + 1, :] = adv
        local_ref[3 * rows + s : 3 * rows + s + 1, :] = ret_ref[s : s + 1, :]
        refs = jnp.where(slot == 0, wide_ref[pl.ds(s, dp, stride=rows), :], 0.0)
        rets = jnp.where(slot == group, jnp.broadcast_to(ret_ref[s : s + 1, :], (dp, LANES)), 0.0)
        lives = jnp.where(slot == group, jnp.broadcast_to(live, (dp, LANES)), 0.0)
        block = jnp.where(spot == rows, fold(refs, tl), 0.0)
        block = jnp.where(spot == rows + 1, fold(rets, tl), block)
        block = jnp.where(spot == rows + 2, fold(lives, tl), block)
        last = (rows + 3) * tl
        block = jnp.where(place == last, jnp.sum(live, axis=1, keepdims=True), block)
        block = jnp.where(place == last + 1, jnp.sum(gain, axis=1, keepdims=True), block)
        block = jnp.where(place == last + 2, jnp.sum(gain * adv, axis=1, keepdims=True), block)
        block = jnp.where(place == last + 3, prompt, block)
        blocks.append(block)
    for copy in copies[:2]:
        copy.wait()
    weights = w_ref[...][None, :].astype(F32)
    flat = []
    for h in range(rows):
        wide = critic_ref[h * LANES : (h + 1) * LANES, :].astype(F32) * weights
        flat.append(jnp.sum(jnp.transpose(lane_sums(wide)), axis=0, keepdims=True))
    for h in range(rows):
        stats_ref[3 * rows + h : 3 * rows + h + 1, :] = flat[h]
    for s in range(rows):
        block = blocks[s]
        for h in range(rows):
            line = jnp.broadcast_to(flat[h], (dp, LANES))
            block = jnp.where((h * LANES + lane) // tl == group * rows + s, line, block)
        for j in range(tn):
            send_ref[pl.ds(j * rows + s, dp, stride=tn * rows), :] = block
    out = pltpu.make_async_copy(send_ref, send_hbm, sems.at[sems.shape[0] - 1])
    out.start()

    @pl.when(is_early())
    def _():
        run_stats(ids_hbm, logits_hbm, stats_ref, *scratch, sems)

    out.wait()


def run_stats(
    ids_hbm, logits_hbm, out_ref,
    logits_ref, ids_ref, ids_smem, here_ref, top_ref, sum_ref, hit_ref, sems,
):
    rows, tokens, width = logits_ref.shape
    chunks = width // LANES
    steps = STEPS
    step = tokens // steps
    blocks = [(s, k) for s in range(rows) for k in range(steps)]
    copies = [
        pltpu.make_async_copy(
            logits_hbm.at[s, pl.ds(k * step, step)],
            logits_ref.at[s, pl.ds(k * step, step)],
            sems.at[s * steps + k],
        )
        for s, k in blocks
    ]
    ids_copies = [
        pltpu.make_async_copy(ids_hbm, ids_ref, sems.at[rows * steps]),
        pltpu.make_async_copy(ids_hbm, ids_smem, sems.at[rows * steps + 1]),
    ]
    for copy in ids_copies + copies:
        copy.start()
    start = lax.axis_index("tensor") * width
    lane = lax.broadcasted_iota(jnp.int32, (tokens, LANES), 1)
    for copy in ids_copies:
        copy.wait()
    for s in range(rows):
        ids = jnp.broadcast_to(ids_ref[s : s + 1, :].astype(F32), (LANES, tokens))
        shifted = jnp.transpose(ids).astype(jnp.int32) - start
        here = (lane == (shifted & (LANES - 1))) & (shifted >= 0) & (shifted < width)
        here_ref[s] = here.astype(F32)

    def part_of(n, c):
        s, k = blocks[n]
        return logits_ref[s, k * step : (k + 1) * step, c * LANES : (c + 1) * LANES]

    def shift_of(n):
        copies[n].wait()
        return jnp.max(part_of(n, 0).astype(F32), axis=1, keepdims=True)

    over_lanes = (((1,), (1,)), ((), ()))
    ones = jnp.ones((16, LANES), jnp.bfloat16)

    def sum_row(s):
        return jnp.sum(jnp.transpose(sum_ref[s]), axis=0, keepdims=True)

    def top_row(s):
        return lax.dot_general(
            ones * (1.0 / LANES), top_ref[s], over_lanes, preferred_element_type=F32
        )[0:1, :]

    row8 = lax.broadcasted_iota(jnp.int32, (8, LANES), 0)
    worst = jnp.zeros((8, LANES), F32)
    top = shift_of(0)
    for n, (s, k) in enumerate(blocks):
        later = shift_of(n + 1) if n + 1 < len(blocks) else None
        at = slice(k * step, (k + 1) * step)
        total = jnp.zeros((step, LANES), F32)
        for c in range(chunks):
            total = total + jnp.exp(part_of(n, c).astype(F32) - top)
        top_ref[s, at, :] = jnp.broadcast_to(top, (step, LANES)).astype(jnp.bfloat16)
        sum_ref[s, at, :] = total
        for q in range(step // 8):
            worst = jnp.maximum(worst, total[q * 8 : (q + 1) * 8, :])
            first = k * step + q * 8
            hit = jnp.zeros((8, LANES), F32)
            for r in range(8):
                chunk = jnp.clip((ids_smem[s, first + r] - start) >> 7, 0, chunks - 1)
                cols = pl.ds(pl.multiple_of(chunk * LANES, LANES), LANES)
                x = logits_ref[s, first : first + 8, cols].astype(F32)
                hit = jnp.where(row8 == r, x, hit)
            here = here_ref[s, first : first + 8, :] > 0.0
            hit_ref[s, first : first + 8, :] = jnp.where(here, hit, 0.0)
        top = later
        if k == steps - 1:
            hits = lax.dot_general(
                ones, hit_ref[s].astype(jnp.bfloat16), over_lanes, preferred_element_type=F32
            )
            out_ref[s : s + 1, :] = top_row(s)
            out_ref[rows + s : rows + s + 1, :] = sum_row(s)
            out_ref[2 * rows + s : 2 * rows + s + 1, :] = hits[0:1, :]

    @pl.when(jnp.logical_not(jnp.max(worst) < 1e30))
    def _():
        for s in range(rows):

            def again(k, carry, s=s):
                at = pl.ds(pl.multiple_of(k * 32, 32), 32)
                top = logits_ref[s, at, 0:LANES]
                for c in range(1, chunks):
                    top = jnp.maximum(top, logits_ref[s, at, c * LANES : (c + 1) * LANES])
                top = jnp.max(top.astype(F32), axis=1, keepdims=True)
                total = jnp.zeros((32, LANES), F32)
                for c in range(chunks):
                    x = logits_ref[s, at, c * LANES : (c + 1) * LANES].astype(F32)
                    total = total + jnp.exp(x - top)
                top_ref[s, at, :] = jnp.broadcast_to(top, (32, LANES)).astype(jnp.bfloat16)
                sum_ref[s, at, :] = total
                return carry

            lax.fori_loop(0, tokens // 32, again, 0)
            out_ref[s : s + 1, :] = top_row(s)
            out_ref[rows + s : rows + s + 1, :] = sum_row(s)


def stats_kernel(ids_hbm, early_ref, logits_hbm, out_ref, *scratch):
    out_ref[...] = early_ref[...]

    @pl.when(jnp.logical_not(is_early()))
    def _():
        run_stats(ids_hbm, logits_hbm, out_ref, *scratch)


def merge_kernel(dims, old_ref, *refs):
    dp, tn, rows, tl = dims
    stats, (logprob_ref, ratio_ref, tile_ref) = refs[:tn], refs[tn:]
    seqs = dp * rows
    tops = [stat[0:rows, :] for stat in stats]
    row_max = functools.reduce(jnp.maximum, tops)
    exp_sum = sum(
        stat[rows : 2 * rows, :] * jnp.exp(top - row_max) for stat, top in zip(stats, tops)
    )
    target = sum(stat[2 * rows : 3 * rows, :] for stat in stats)
    logprob = target - (row_max + jnp.log(exp_sum))
    logprob_ref[...] = logprob
    ratio_ref[...] = jnp.exp(jnp.clip(logprob - old_ref[...], -20.0, 20.0))

    order = lax.broadcasted_iota(jnp.int32, (seqs, LANES), 0)
    seq = (order % dp) * rows + order // dp
    lane = lax.broadcasted_iota(jnp.int32, (seqs, LANES), 1)
    tile = jnp.zeros((seqs, LANES), F32)
    for h in range(rows):
        line = sum(stat[3 * rows + h : 3 * rows + h + 1, :] for stat in stats)
        here = (h * LANES + lane) // tl == seq
        tile = jnp.where(here, jnp.broadcast_to(line, (seqs, LANES)), tile)
    tile_ref[...] = jnp.transpose(fold(tile, tl))[0:tl, :]


def post_kernel(
    dims, recv_ref, w_ref, local_ref, logprob_ref, ratio_ref, tile_ref,
    loss_hbm, grad_hbm, loss_ref, grad_ref, sems,
):
    dp, tn, rows, tl = dims
    seqs = dp * rows
    group, lane, slot = group_grid(dp, tl)
    parts = [
        [recv_ref[pl.ds(j * rows + s, dp, stride=tn * rows), :] for j in range(tn)]
        for s in range(rows)
    ]
    back = LANES - (lax.axis_index("dp") * (rows * tl)) % LANES
    firsts = [pltpu.roll(part[0], back, 1) for part in parts]
    every = [pltpu.roll(sum(part[1:], part[0]), back, 1) for part in parts]

    def row_of(x, k):
        apart = pltpu.roll(x, 0, 1, stride=tl, stride_axis=0)
        row = jnp.sum(jnp.where(slot == (group + k) % dp, apart, 0.0), axis=0, keepdims=True)
        return pltpu.roll(row, LANES - k * tl, 1) if k else row

    spot = (rows + 3) * tl
    prompts = [first[:, spot + 3 : spot + 4] for first in firsts]

    columns = jnp.transpose(jnp.concatenate(firsts, axis=0))
    at = (rows + 1) * tl
    coeff = (
        32.0 * columns[at + tl : at + 2 * tl, :] * (tile_ref[...] - columns[at : at + tl, :])
    )
    weights = w_ref[...][None, :].astype(F32)
    pieces = sems.shape[0] - 1
    piece = seqs // pieces
    copies = []
    for k in range(pieces):
        for b in range(k * piece, (k + 1) * piece):
            at = (b % rows) * dp + b // rows
            grad_ref[b] = (coeff[:, at : at + 1] * weights).astype(grad_ref.dtype)
        at = pl.ds(k * piece, piece)
        copies.append(pltpu.make_async_copy(grad_ref.at[at], grad_hbm.at[at], sems.at[k]))
        copies[-1].start()

    for s in range(rows):
        value_pred = row_of(every[s], s)
        ref_row = row_of(firsts[s], rows)
        own = local_ref[rows + s : rows + s + 1, 0:1]
        sums = jnp.zeros((1, LANES), F32)
        for first, prompt in zip(firsts, prompts):
            sums += jnp.sum(jnp.where(prompt == own, first, 0.0), axis=0, keepdims=True)
        count = jnp.maximum(sums, 1.0)
        total = pltpu.roll(sums, LANES - 1, 1)
        square = pltpu.roll(sums, LANES - 2, 1)
        mean = total / count
        scale = lax.rsqrt((square - mean * total) / count + 1.0)
        adv = local_ref[2 * rows + s : 2 * rows + s + 1, :]
        whitened = (adv - mean[:, spot : spot + 1]) * scale[:, spot : spot + 1]

        ratio = ratio_ref[s : s + 1, :]
        surrogate = jnp.maximum(-whitened * ratio, -whitened * jnp.clip(ratio, 0.8, 1.2))
        surrogate = jnp.where(whitened < 0.0, jnp.minimum(surrogate, -3.0 * whitened), surrogate)
        drift = jnp.clip(ref_row - logprob_ref[s : s + 1, :], -20.0, 20.0)
        penalty = jnp.clip(jnp.exp(drift) - drift - 1.0, -10.0, 10.0)
        error = value_pred - local_ref[3 * rows + s : 3 * rows + s + 1, :]
        live = local_ref[s : s + 1, :]
        loss_ref[s : s + 1, :] = live * (surrogate + 0.1 * penalty + 0.25 * error * error)
    copies.append(pltpu.make_async_copy(loss_ref, loss_hbm, sems.at[pieces]))
    copies[-1].start()
    for copy in copies:
        copy.wait()


def per_device(
    logits,
    token_ids,
    response_mask,
    lengths,
    prompt_of,
    old_logprob,
    ref_logprob,
    advantages,
    returns,
    critic_hidden,
    value_weight,
):
    rows, tokens, width = logits.shape
    seqs, tl, feat = critic_hidden.shape
    dp, tn = lax.axis_size("dp"), lax.axis_size("tensor")
    dims = (dp, tn, rows, tl)
    if tokens != LANES or width % LANES or (rows + 3) * tl + 4 > LANES or LANES % tl or tn & (tn - 1):
        raise ValueError("unsupported shapes")
    vmem = pl.BlockSpec(memory_space=pltpu.VMEM)
    hbm = pl.BlockSpec(memory_space=pltpu.HBM)

    def grant(mib):
        return pltpu.CompilerParams(vmem_limit_bytes=mib << 20)

    stats_scratch = [
        pltpu.VMEM(logits.shape, logits.dtype),
        pltpu.VMEM((rows, tokens), jnp.int32),
        pltpu.SMEM((rows, tokens), jnp.int32),
        pltpu.VMEM((rows, tokens, LANES), F32),
        pltpu.VMEM((rows, tokens, LANES), jnp.bfloat16),
        pltpu.VMEM((rows, tokens, LANES), F32),
        pltpu.VMEM((rows, tokens, LANES), F32),
    ]
    copies = rows * STEPS + 2
    send, early, local = pl.pallas_call(
        functools.partial(pre_kernel, dims),
        name="pre",
        out_shape=(
            jax.ShapeDtypeStruct((dp * tn * rows, LANES), F32),
            jax.ShapeDtypeStruct((4 * rows, LANES), F32),
            jax.ShapeDtypeStruct((4 * rows, LANES), F32),
        ),
        in_specs=[hbm] * 10,
        out_specs=(hbm, vmem, vmem),
        scratch_shapes=[
            pltpu.SMEM(lengths.shape, jnp.int32),
            pltpu.SMEM(prompt_of.shape, jnp.int32),
            pltpu.VMEM((seqs * tl, feat), jnp.bfloat16),
            pltpu.VMEM((feat,), jnp.bfloat16),
            pltpu.VMEM((seqs, tl), jnp.bfloat16),
            pltpu.VMEM((rows, LANES), F32),
            pltpu.VMEM((rows, LANES), jnp.int32),
            pltpu.VMEM((rows, LANES), F32),
            pltpu.VMEM((dp * tn * rows, LANES), F32),
            pltpu.VMEM((seqs, LANES), F32),
            pltpu.SemaphoreType.DMA((max(copies, 8) + 1,)),
            *stats_scratch,
        ],
        compiler_params=grant(10),
    )(
        *in_hbm(
            lengths, prompt_of, critic_hidden.reshape(seqs * tl, feat), value_weight, ref_logprob,
            returns, response_mask, advantages, token_ids, logits,
        )
    )
    received = lax.all_to_all(
        send.reshape(dp * tn, rows, LANES), ("dp", "tensor"), 0, 0, tiled=True
    ).reshape(dp * tn * rows, LANES)

    stats = pl.pallas_call(
        stats_kernel,
        name="stats",
        out_shape=jax.ShapeDtypeStruct((4 * rows, LANES), F32),
        in_specs=[hbm, vmem, hbm],
        out_specs=vmem,
        scratch_shapes=[*stats_scratch, pltpu.SemaphoreType.DMA((copies,))],
        compiler_params=grant(8),
        cost_estimate=pl.CostEstimate(
            flops=8 * logits.size, bytes_accessed=2 * logits.size, transcendentals=logits.size
        ),
    )(*in_hbm(token_ids), early, *in_hbm(logits))
    shards = [stats] + [
        lax.ppermute(stats, "tensor", [(t, t ^ k) for t in range(tn)])
        for k in reversed(range(1, tn))
    ]

    merged = pl.pallas_call(
        functools.partial(merge_kernel, dims),
        name="merge",
        out_shape=(
            jax.ShapeDtypeStruct((rows, LANES), F32),
            jax.ShapeDtypeStruct((rows, LANES), F32),
            jax.ShapeDtypeStruct((tl, seqs), F32),
        ),
        in_specs=[vmem] * (1 + tn),
        out_specs=(vmem,) * 3,
        compiler_params=grant(4),
    )(old_logprob, *shards)

    return pl.pallas_call(
        functools.partial(post_kernel, dims),
        name="post",
        out_shape=(
            jax.ShapeDtypeStruct((rows, tokens), F32),
            jax.ShapeDtypeStruct((seqs, tl, feat), jnp.bfloat16),
        ),
        in_specs=[vmem] * 6,
        out_specs=(hbm, hbm),
        scratch_shapes=[
            pltpu.VMEM((rows, tokens), F32),
            pltpu.VMEM((seqs, tl, feat), jnp.bfloat16),
            pltpu.SemaphoreType.DMA((3,)),
        ],
        compiler_params=grant(6),
    )(received, value_weight, local, *merged)


def solution(mesh):
    in_specs = (
        P("dp", None, "tensor"),
        P("dp", None),
        P("dp", None),
        P("dp"),
        P("dp"),
        P("dp", None),
        P(None, "dp"),
        P("dp", None),
        P("dp", None),
        P(None, "dp", "tensor"),
        P("tensor"),
    )
    out_specs = (P("dp", None), P(None, "dp", "tensor"))
    return jax.shard_map(
        per_device, mesh=mesh, in_specs=in_specs, out_specs=out_specs, check_vma=False
    )
```

```python
import functools

import jax
import jax.numpy as jnp
from jax import lax
from jax.experimental import pallas as pl
from jax.experimental.pallas import tpu as pltpu
from jax.sharding import PartitionSpec as P

LANES = 128
STEPS = 4
NOT_LIVE = 1e9
F32 = jnp.float32


def fold(x, period):
    shift = LANES // 2
    while shift >= period:
        x = x + pltpu.roll(x, shift, 1)
        shift //= 2
    return x


def in_hbm(*arrays):
    return [pltpu.with_memory_space_constraint(x, pltpu.HBM) for x in arrays]


def live_row(rmask_ref, len_ref, s):
    position = lax.broadcasted_iota(jnp.int32, (1, LANES), 1)
    return jnp.where(position < len_ref[s], rmask_ref[s : s + 1, :], 0).astype(F32)


def group_grid(dp, tl):
    group = lax.broadcasted_iota(jnp.int32, (dp, LANES), 0)
    lane = lax.broadcasted_iota(jnp.int32, (dp, LANES), 1)
    return group, lane, lane // tl


def is_early():
    return lax.axis_index("dp") == 0


def lane_sums(wide):
    total = wide[:, 0:LANES]
    whole = wide.shape[1] // LANES
    for c in range(1, whole):
        total = total + wide[:, c * LANES : (c + 1) * LANES]
    left = wide.shape[1] - whole * LANES
    if left:
        pad = jnp.zeros((wide.shape[0], LANES - left), F32)
        total = total + jnp.concatenate([wide[:, whole * LANES :], pad], axis=1)
    return total


def pre_kernel(
    dims, len_hbm, prompt_hbm, critic_hbm, w_hbm, refl_hbm, ret_hbm, rmask_hbm, adv_hbm,
    ids_hbm, logits_hbm,
    send_hbm, stats_ref, local_ref,
    len_ref, prompt_ref, critic_ref, w_ref, reflp_ref, ret_ref, rmask_ref, adv_ref, send_ref,
    wide_ref, sems, *scratch,
):
    dp, tn, rows, tl = dims
    pairs = (
        (w_hbm, w_ref), (critic_hbm, critic_ref), (rmask_hbm, rmask_ref), (adv_hbm, adv_ref),
        (ret_hbm, ret_ref), (refl_hbm, reflp_ref), (len_hbm, len_ref), (prompt_hbm, prompt_ref),
    )
    copies = [pltpu.make_async_copy(a, b, sems.at[k]) for k, (a, b) in enumerate(pairs)]
    for copy in copies[::-1]:
        copy.start()
    for copy in copies[2:]:
        copy.wait()
    wide_ref[:, 0:tl] = reflp_ref[...].astype(F32)
    group, lane, slot = group_grid(dp, tl)
    place = (lane - group * (rows * tl)) & (LANES - 1)
    spot = place // tl
    block = jnp.zeros((dp, LANES), F32)
    for s in range(rows):
        live = live_row(rmask_ref, len_ref, s)
        adv = adv_ref[s : s + 1, :]
        gain = live * adv
        prompt = prompt_ref[s].astype(F32)
        local_ref[s : s + 1, :] = live
        local_ref[rows + s : rows + s + 1, :] = jnp.zeros((1, LANES), F32) + prompt
        local_ref[2 * rows + s : 2 * rows + s + 1, :] = adv
        local_ref[3 * rows + s : 3 * rows + s + 1, :] = ret_ref[s : s + 1, :]
        refs = jnp.where(slot == 0, wide_ref[pl.ds(s, dp, stride=rows), :], 0.0)
        rets = jnp.where(live > 0.0, ret_ref[s : s + 1, :], NOT_LIVE)
        rets = jnp.where(slot == group, jnp.broadcast_to(rets, (dp, LANES)), 0.0)
        block = jnp.where(spot == rows + s, fold(refs, tl), block)
        block = jnp.where(spot == 2 * rows + s, fold(rets, tl), block)
        last = 3 * rows * tl + 4 * s
        block = jnp.where(place == last, jnp.sum(live, axis=1, keepdims=True), block)
        block = jnp.where(place == last + 1, jnp.sum(gain, axis=1, keepdims=True), block)
        block = jnp.where(place == last + 2, jnp.sum(gain * adv, axis=1, keepdims=True), block)
        block = jnp.where(place == last + 3, prompt, block)
    for copy in copies[:2]:
        copy.wait()
    weights = w_ref[...][None, :].astype(F32)
    flat = []
    for h in range(rows):
        wide = critic_ref[h * LANES : (h + 1) * LANES, :].astype(F32) * weights
        flat.append(jnp.sum(jnp.transpose(lane_sums(wide)), axis=0, keepdims=True))
    for h in range(rows):
        stats_ref[3 * rows + h : 3 * rows + h + 1, :] = flat[h]
    for h in range(rows):
        line = jnp.broadcast_to(flat[h], (dp, LANES))
        block = jnp.where((h * LANES + lane) // (rows * tl) == group, line, block)
    for j in range(tn):
        send_ref[pl.ds(j, dp, stride=tn), :] = block
    out = pltpu.make_async_copy(send_ref, send_hbm, sems.at[sems.shape[0] - 1])
    out.start()

    @pl.when(is_early())
    def _():
        run_stats(ids_hbm, logits_hbm, stats_ref, *scratch, sems)

    out.wait()


def run_stats(
    ids_hbm, logits_hbm, out_ref,
    logits_ref, ids_ref, ids_smem, here_ref, top_ref, sum_ref, hit_ref, sems,
):
    rows, tokens, width = logits_ref.shape
    chunks = width // LANES
    steps = STEPS
    step = tokens // steps
    blocks = [(s, k) for s in range(rows) for k in range(steps)]
    copies = [
        pltpu.make_async_copy(
            logits_hbm.at[s, pl.ds(k * step, step)],
            logits_ref.at[s, pl.ds(k * step, step)],
            sems.at[s * steps + k],
        )
        for s, k in blocks
    ]
    ids_copies = [
        pltpu.make_async_copy(ids_hbm, ids_ref, sems.at[rows * steps]),
        pltpu.make_async_copy(ids_hbm, ids_smem, sems.at[rows * steps + 1]),
    ]
    for copy in ids_copies + copies:
        copy.start()
    start = lax.axis_index("tensor") * width
    lane = lax.broadcasted_iota(jnp.int32, (tokens, LANES), 1)
    for copy in ids_copies:
        copy.wait()
    for s in range(rows):
        ids = jnp.broadcast_to(ids_ref[s : s + 1, :].astype(F32), (LANES, tokens))
        shifted = jnp.transpose(ids).astype(jnp.int32) - start
        here = (lane == (shifted & (LANES - 1))) & (shifted >= 0) & (shifted < width)
        here_ref[s] = here.astype(F32)

    def part_of(n, c):
        s, k = blocks[n]
        return logits_ref[s, k * step : (k + 1) * step, c * LANES : (c + 1) * LANES]

    def shift_of(n):
        copies[n].wait()
        return jnp.max(part_of(n, 0).astype(F32), axis=1, keepdims=True)

    over_lanes = (((1,), (1,)), ((), ()))
    ones = jnp.ones((16, LANES), jnp.bfloat16)

    def sum_row(s):
        return jnp.sum(jnp.transpose(sum_ref[s]), axis=0, keepdims=True)

    def top_row(s):
        return lax.dot_general(
            ones * (1.0 / LANES), top_ref[s], over_lanes, preferred_element_type=F32
        )[0:1, :]

    row8 = lax.broadcasted_iota(jnp.int32, (8, LANES), 0)
    worst = jnp.zeros((8, LANES), F32)
    top = shift_of(0)
    for n, (s, k) in enumerate(blocks):
        later = shift_of(n + 1) if n + 1 < len(blocks) else None
        at = slice(k * step, (k + 1) * step)
        total = jnp.zeros((step, LANES), F32)
        for c in range(chunks):
            total = total + jnp.exp(part_of(n, c).astype(F32) - top)
        top_ref[s, at, :] = jnp.broadcast_to(top, (step, LANES)).astype(jnp.bfloat16)
        sum_ref[s, at, :] = total
        for q in range(step // 8):
            worst = jnp.maximum(worst, total[q * 8 : (q + 1) * 8, :])
            first = k * step + q * 8
            hit = jnp.zeros((8, LANES), F32)
            for r in range(8):
                chunk = jnp.clip((ids_smem[s, first + r] - start) >> 7, 0, chunks - 1)
                cols = pl.ds(pl.multiple_of(chunk * LANES, LANES), LANES)
                x = logits_ref[s, first : first + 8, cols].astype(F32)
                hit = jnp.where(row8 == r, x, hit)
            here = here_ref[s, first : first + 8, :] > 0.0
            hit_ref[s, first : first + 8, :] = jnp.where(here, hit, 0.0)
        top = later
        if k == steps - 1:
            hits = lax.dot_general(
                ones, hit_ref[s].astype(jnp.bfloat16), over_lanes, preferred_element_type=F32
            )
            out_ref[s : s + 1, :] = top_row(s)
            out_ref[rows + s : rows + s + 1, :] = sum_row(s)
            out_ref[2 * rows + s : 2 * rows + s + 1, :] = hits[0:1, :]

    @pl.when(jnp.logical_not(jnp.max(worst) < 1e30))
    def _():
        for s in range(rows):

            def again(k, carry, s=s):
                at = pl.ds(pl.multiple_of(k * 32, 32), 32)
                top = logits_ref[s, at, 0:LANES]
                for c in range(1, chunks):
                    top = jnp.maximum(top, logits_ref[s, at, c * LANES : (c + 1) * LANES])
                top = jnp.max(top.astype(F32), axis=1, keepdims=True)
                total = jnp.zeros((32, LANES), F32)
                for c in range(chunks):
                    x = logits_ref[s, at, c * LANES : (c + 1) * LANES].astype(F32)
                    total = total + jnp.exp(x - top)
                top_ref[s, at, :] = jnp.broadcast_to(top, (32, LANES)).astype(jnp.bfloat16)
                sum_ref[s, at, :] = total
                return carry

            lax.fori_loop(0, tokens // 32, again, 0)
            out_ref[s : s + 1, :] = top_row(s)
            out_ref[rows + s : rows + s + 1, :] = sum_row(s)


def stats_kernel(ids_hbm, early_ref, logits_hbm, out_ref, *scratch):
    out_ref[...] = early_ref[...]

    @pl.when(jnp.logical_not(is_early()))
    def _():
        run_stats(ids_hbm, logits_hbm, out_ref, *scratch)


def merge_kernel(dims, old_ref, *refs):
    dp, tn, rows, tl = dims
    stats, (logprob_ref, ratio_ref, tile_ref) = refs[:tn], refs[tn:]
    tops = [stat[0:rows, :] for stat in stats]
    row_max = functools.reduce(jnp.maximum, tops)
    exp_sum = sum(
        stat[rows : 2 * rows, :] * jnp.exp(top - row_max) for stat, top in zip(stats, tops)
    )
    target = sum(stat[2 * rows : 3 * rows, :] for stat in stats)
    logprob = target - (row_max + jnp.log(exp_sum))
    logprob_ref[...] = logprob
    ratio_ref[...] = jnp.exp(jnp.clip(logprob - old_ref[...], -20.0, 20.0))

    group, lane, slot = group_grid(dp, tl)
    for s in range(rows):
        tile = jnp.zeros((dp, LANES), F32)
        for h in range(rows):
            line = sum(stat[3 * rows + h : 3 * rows + h + 1, :] for stat in stats)
            here = (h * LANES + lane) // tl == group * rows + s
            tile = jnp.where(here, jnp.broadcast_to(line, (dp, LANES)), tile)
        tile_ref[s * tl : (s + 1) * tl, :] = jnp.transpose(fold(tile, tl))[0:tl, :]


def post_kernel(
    dims, recv_ref, w_ref, local_ref, logprob_ref, ratio_ref, tile_ref,
    loss_hbm, grad_hbm, loss_ref, grad_ref, sems,
):
    dp, tn, rows, tl = dims
    seqs = dp * rows
    group, lane, slot = group_grid(dp, tl)
    parts = [recv_ref[pl.ds(j, dp, stride=tn), :] for j in range(tn)]
    back = LANES - (lax.axis_index("dp") * (rows * tl)) % LANES
    first = pltpu.roll(parts[0], back, 1)
    every = pltpu.roll(sum(parts[1:], parts[0]), back, 1)

    def row_of(x, k):
        apart = pltpu.roll(x, 0, 1, stride=tl, stride_axis=0)
        row = jnp.sum(jnp.where(slot == (group + k) % dp, apart, 0.0), axis=0, keepdims=True)
        return pltpu.roll(row, LANES - k * tl, 1) if k else row

    targets = jnp.transpose(first)[2 * rows * tl : 3 * rows * tl, :]
    coeff = jnp.where(targets < 0.5 * NOT_LIVE, 32.0 * (tile_ref[...] - targets), 0.0)
    weights = w_ref[...][None, :].astype(F32)
    pieces = sems.shape[0] - 1
    piece = seqs // pieces
    copies = []
    for k in range(pieces):
        for b in range(k * piece, (k + 1) * piece):
            column = coeff[b % rows * tl : (b % rows + 1) * tl, b // rows : b // rows + 1]
            grad_ref[b] = (column * weights).astype(grad_ref.dtype)
        at = pl.ds(k * piece, piece)
        copies.append(pltpu.make_async_copy(grad_ref.at[at], grad_hbm.at[at], sems.at[k]))
        copies[-1].start()

    spot = 3 * rows * tl
    for s in range(rows):
        value_pred = row_of(every, s)
        ref_row = row_of(first, rows + s)
        own = local_ref[rows + s : rows + s + 1, 0:1]
        sums = jnp.zeros((1, LANES), F32)
        for q in range(rows):
            same = first[:, spot + 4 * q + 3 : spot + 4 * q + 4] == own
            part = jnp.sum(jnp.where(same, first, 0.0), axis=0, keepdims=True)
            sums += pltpu.roll(part, LANES - 4 * q, 1) if q else part
        count = jnp.maximum(sums, 1.0)
        total = pltpu.roll(sums, LANES - 1, 1)
        square = pltpu.roll(sums, LANES - 2, 1)
        mean = total / count
        scale = lax.rsqrt((square - mean * total) / count + 1.0)
        adv = local_ref[2 * rows + s : 2 * rows + s + 1, :]
        whitened = (adv - mean[:, spot : spot + 1]) * scale[:, spot : spot + 1]

        ratio = ratio_ref[s : s + 1, :]
        surrogate = jnp.maximum(-whitened * ratio, -whitened * jnp.clip(ratio, 0.8, 1.2))
        surrogate = jnp.where(whitened < 0.0, jnp.minimum(surrogate, -3.0 * whitened), surrogate)
        drift = jnp.clip(ref_row - logprob_ref[s : s + 1, :], -20.0, 20.0)
        penalty = jnp.clip(jnp.exp(drift) - drift - 1.0, -10.0, 10.0)
        error = value_pred - local_ref[3 * rows + s : 3 * rows + s + 1, :]
        live = local_ref[s : s + 1, :]
        loss_ref[s : s + 1, :] = live * (surrogate + 0.1 * penalty + 0.25 * error * error)
    copies.append(pltpu.make_async_copy(loss_ref, loss_hbm, sems.at[pieces]))
    copies[-1].start()
    for copy in copies:
        copy.wait()


def per_device(
    logits,
    token_ids,
    response_mask,
    lengths,
    prompt_of,
    old_logprob,
    ref_logprob,
    advantages,
    returns,
    critic_hidden,
    value_weight,
):
    rows, tokens, width = logits.shape
    seqs, tl, feat = critic_hidden.shape
    dp, tn = lax.axis_size("dp"), lax.axis_size("tensor")
    dims = (dp, tn, rows, tl)
    if tokens != LANES or width % LANES or 3 * rows * tl + 4 * rows > LANES or LANES % (rows * tl) or tn & (tn - 1):
        raise ValueError("unsupported shapes")
    vmem = pl.BlockSpec(memory_space=pltpu.VMEM)
    hbm = pl.BlockSpec(memory_space=pltpu.HBM)

    def grant(mib):
        return pltpu.CompilerParams(vmem_limit_bytes=mib << 20)

    stats_scratch = [
        pltpu.VMEM(logits.shape, logits.dtype),
        pltpu.VMEM((rows, tokens), jnp.int32),
        pltpu.SMEM((rows, tokens), jnp.int32),
        pltpu.VMEM((rows, tokens, LANES), F32),
        pltpu.VMEM((rows, tokens, LANES), jnp.bfloat16),
        pltpu.VMEM((rows, tokens, LANES), F32),
        pltpu.VMEM((rows, tokens, LANES), F32),
    ]
    copies = rows * STEPS + 2
    send, early, local = pl.pallas_call(
        functools.partial(pre_kernel, dims),
        name="pre",
        out_shape=(
            jax.ShapeDtypeStruct((dp * tn, LANES), F32),
            jax.ShapeDtypeStruct((4 * rows, LANES), F32),
            jax.ShapeDtypeStruct((4 * rows, LANES), F32),
        ),
        in_specs=[hbm] * 10,
        out_specs=(hbm, vmem, vmem),
        scratch_shapes=[
            pltpu.SMEM(lengths.shape, jnp.int32),
            pltpu.SMEM(prompt_of.shape, jnp.int32),
            pltpu.VMEM((seqs * tl, feat), jnp.bfloat16),
            pltpu.VMEM((feat,), jnp.bfloat16),
            pltpu.VMEM((seqs, tl), jnp.bfloat16),
            pltpu.VMEM((rows, LANES), F32),
            pltpu.VMEM((rows, LANES), jnp.int32),
            pltpu.VMEM((rows, LANES), F32),
            pltpu.VMEM((dp * tn, LANES), F32),
            pltpu.VMEM((seqs, LANES), F32),
            pltpu.SemaphoreType.DMA((max(copies, 8) + 1,)),
            *stats_scratch,
        ],
        compiler_params=grant(10),
    )(
        *in_hbm(
            lengths, prompt_of, critic_hidden.reshape(seqs * tl, feat), value_weight, ref_logprob,
            returns, response_mask, advantages, token_ids, logits,
        )
    )
    received = lax.all_to_all(send, ("dp", "tensor"), 0, 0, tiled=True)

    stats = pl.pallas_call(
        stats_kernel,
        name="stats",
        out_shape=jax.ShapeDtypeStruct((4 * rows, LANES), F32),
        in_specs=[hbm, vmem, hbm],
        out_specs=vmem,
        scratch_shapes=[*stats_scratch, pltpu.SemaphoreType.DMA((copies,))],
        compiler_params=grant(8),
        cost_estimate=pl.CostEstimate(
            flops=8 * logits.size, bytes_accessed=2 * logits.size, transcendentals=logits.size
        ),
    )(*in_hbm(token_ids), early, *in_hbm(logits))
    shards = [stats] + [
        lax.ppermute(stats, "tensor", [(t, t ^ k) for t in range(tn)])
        for k in reversed(range(1, tn))
    ]

    merged = pl.pallas_call(
        functools.partial(merge_kernel, dims),
        name="merge",
        out_shape=(
            jax.ShapeDtypeStruct((rows, LANES), F32),
            jax.ShapeDtypeStruct((rows, LANES), F32),
            jax.ShapeDtypeStruct((rows * tl, dp), F32),
        ),
        in_specs=[vmem] * (1 + tn),
        out_specs=(vmem,) * 3,
        compiler_params=grant(4),
    )(old_logprob, *shards)

    return pl.pallas_call(
        functools.partial(post_kernel, dims),
        name="post",
        out_shape=(
            jax.ShapeDtypeStruct((rows, tokens), F32),
            jax.ShapeDtypeStruct((seqs, tl, feat), jnp.bfloat16),
        ),
        in_specs=[vmem] * 6,
        out_specs=(hbm, hbm),
        scratch_shapes=[
            pltpu.VMEM((rows, tokens), F32),
            pltpu.VMEM((seqs, tl, feat), jnp.bfloat16),
            pltpu.SemaphoreType.DMA((3,)),
        ],
        compiler_params=grant(6),
    )(received, value_weight, local, *merged)


def solution(mesh):
    in_specs = (
        P("dp", None, "tensor"),
        P("dp", None),
        P("dp", None),
        P("dp"),
        P("dp"),
        P("dp", None),
        P(None, "dp"),
        P("dp", None),
        P("dp", None),
        P(None, "dp", "tensor"),
        P("tensor"),
    )
    out_specs = (P("dp", None), P(None, "dp", "tensor"))
    return jax.shard_map(
        per_device, mesh=mesh, in_specs=in_specs, out_specs=out_specs, check_vma=False
    )
```
